8 devices in a mesh: dp: 1 (over z), tp: 8 (over x, y, core).
Axes of the slice: x: 2, y: 2, z: 1, core: 2. Of those that a mesh axis runs over, the one named last changes fastest.
Arguments:
- x: bfloat16 [128, 12288], P('dp')
- w_gate: bfloat16 [12288, 33792], P(None, 'tp')
- w_up: bfloat16 [12288, 33792], P(None, 'tp')
- w_down: bfloat16 [33792, 12288], P('tp')
Outputs:
- output: bfloat16 [128, 12288], P('dp')
All inputs are finite; a program needn't handle non-finite values.
Results may differ from the reference program's by a relative error of at most 0.016.
Values are sent between devices in bfloat16 or wider.
A program may use at most 2 GiB of HBM per device.

```python
import jax
import jax.numpy as jnp

ROWS = 128
D = 12288
FF = 33792


def setup_inputs(seed: int = 0, part: int = 0) -> dict:
    kx, kg, ku, kd = jax.random.split(jax.random.key(seed), 4)
    drawn = {
        "x": jax.random.normal(jax.random.fold_in(kx, part), (ROWS, D), jnp.float32),
        "w_gate": jax.random.normal(kg, (D, FF), jnp.float32) * D**-0.5,
        "w_up": jax.random.normal(ku, (D, FF), jnp.float32) * D**-0.5,
        "w_down": jax.random.normal(kd, (FF, D), jnp.float32) * FF**-0.5,
    }
    return {k: v.astype(jnp.bfloat16) for k, v in drawn.items()}


def reference(x, w_gate, w_up, w_down):
    gate = jnp.dot(x, w_gate, preferred_element_type=jnp.float32)
    up = jnp.dot(x, w_up, preferred_element_type=jnp.float32)
    hidden = (jax.nn.silu(gate) * up).astype(jnp.bfloat16)
    return jnp.dot(hidden, w_down, preferred_element_type=jnp.float32).astype(jnp.bfloat16)
```

```python
import functools

import jax
import jax.numpy as jnp
from jax import lax
from jax.experimental import pallas as pl
from jax.experimental.pallas import tpu as pltpu
from jax.sharding import PartitionSpec as P

MESH = pl.DeviceIdType.MESH
ROWS, D, H = 128, 12288, 4224
KB = 1536
COLS = ((0, 1536), (1536, 1536), (3072, 1152))
NB = 512
CHUNKS = D // NB
SLOTS = 8
HALF = SLOTS // 2
LAGS = (1, 3, 5, 7, 9, 10)


def splits(width):
    return [(at, min(512, width - at)) for at in range(0, width, 512)]


def kernel(x_hbm, g_hbm, u_hbm, d_hbm, out_hbm, xv, hidden, acc_g, acc_u, ring, term, own, send0, recv0, send1, recv1,
           send2, recv2, y, x_sem, ring_sem, s0, r0, s1, r1, s2, r2, s3, r3, s4, r4, s5, r5, out_sem):
    me = lax.axis_index("tp")
    core = lax.rem(me, 2)
    cx, cy = me // 4, lax.rem(me // 2, 2)
    code = 4 * core + 2 * cx + cy
    partner = cx * 4 + cy * 2 + (1 - core)
    nbr_x = (1 - cx) * 4 + cy * 2 + core
    nbr_y = cx * 4 + (1 - cy) * 2 + core

    barrier = pltpu.get_barrier_semaphore()
    for peer in (partner, nbr_x, nbr_y):
        pl.semaphore_signal(barrier, inc=1, device_id={"tp": peer}, device_id_type=MESH)

    def x_copy(p):
        ccx, ccy, ccore = cx, cy, core
        if p & 1:
            ccy = 1 - ccy
        if p & 2:
            ccx = 1 - ccx
        if p & 4:
            ccore = 1 - ccore
        row = pl.multiple_of((4 * ccore + 2 * ccx + ccy) * 16, 16)
        return pltpu.make_async_copy(x_hbm.at[pl.ds(row, 16), :], xv.at[pl.ds(16 * p, 16), :], x_sem.at[p])

    def in_copy(w_hbm, nb, kb, slot):
        at, width = COLS[nb]
        return pltpu.make_async_copy(
            w_hbm.at[pl.ds(pl.multiple_of(kb * KB, KB), KB), pl.ds(at, width)],
            ring.at[slot, :, pl.ds(0, width)],
            ring_sem.at[slot, 0],
        )

    def down_copy(j, slot, r):
        at, depth = COLS[r]
        return pltpu.make_async_copy(
            d_hbm.at[pl.ds(at, depth), pl.ds(pl.multiple_of(j * NB, NB), NB)],
            ring.at[slot, pl.ds(0, depth), pl.ds(r * NB, NB)],
            ring_sem.at[slot, r],
        )

    for p in range(8):
        x_copy(p).start()
    for kb in range(HALF):
        in_copy(g_hbm, 0, kb, 2 * kb).start()
        in_copy(u_hbm, 0, kb, 2 * kb + 1).start()
    for p in range(8):
        x_copy(p).wait()

    for nb, (at, width) in enumerate(COLS):
        acc_g[...] = jnp.zeros_like(acc_g)
        acc_u[...] = jnp.zeros_like(acc_u)
        for late in (False, True):

            def body(t, _, nb=nb, width=width, late=late):
                kb = t + HALF if late else t
                xk = xv[:, pl.ds(pl.multiple_of(kb * KB, KB), KB)]
                for which, (w_hbm, acc) in enumerate(((g_hbm, acc_g), (u_hbm, acc_u))):
                    slot = 2 * t + which
                    in_copy(w_hbm, nb, kb, slot).wait()
                    for c, n in splits(width):
                        acc[:, c : c + n] += jnp.dot(xk, ring[slot, :, c : c + n], preferred_element_type=jnp.float32)
                    if not late:
                        in_copy(w_hbm, nb, kb + HALF, slot).start()
                    elif nb + 1 < len(COLS):
                        in_copy(w_hbm, nb + 1, t, slot).start()
                    else:
                        for r in range(3):
                            down_copy(slot, slot, r).start()
                return 0

            lax.fori_loop(0, HALF, body, 0)
        for c, n in splits(width):
            hidden[:, at + c : at + c + n] = (jax.nn.silu(acc_g[:, c : c + n]) * acc_u[:, c : c + n]).astype(jnp.bfloat16)

    pl.semaphore_wait(barrier, 3)

    def rdma(src, dst, send_sem, recv_sem, peer):
        return pltpu.make_async_remote_copy(
            src_ref=src, dst_ref=dst, send_sem=send_sem, recv_sem=recv_sem, device_id={"tp": peer}, device_id_type=MESH
        )

    def cols(c):
        return pl.ds(pl.multiple_of(c * NB, NB), NB)

    def c0(c):
        return rdma(send0.at[:, cols(c)], recv0.at[:, cols(c)], s0.at[c], r0.at[c], partner)

    def c1(c, odd):
        return rdma(send1.at[:, cols(c)], recv1.at[:, cols(c)], s1.at[c], r1.at[c], nbr_y if odd else nbr_x)

    def c2(c, odd):
        return rdma(send2.at[:, cols(c)], recv2.at[:, cols(c)], s2.at[c], r2.at[c], nbr_x if odd else nbr_y)

    def piece(core_, x_, y_):
        return pl.ds(pl.multiple_of((4 * core_ + 2 * x_ + y_) * 16, 16), 16)

    def c3(c, odd):
        at = y.at[piece(core, cx, cy), cols(c)]
        return rdma(at, at, s3.at[c], r3.at[c], nbr_x if odd else nbr_y)

    def c4(c, odd, second):
        if odd:
            at = y.at[piece(core, 1 - cx if second else cx, cy), cols(c)]
        else:
            at = y.at[piece(core, cx, 1 - cy if second else cy), cols(c)]
        return rdma(at, at, s4.at[c, int(second)], r4.at[c, int(second)], nbr_y if odd else nbr_x)

    def c5(c):
        at = y.at[pl.ds(pl.multiple_of(core * 64, 64), 64), cols(c)]
        return rdma(at, at, s5.at[c], r5.at[c], partner)

    def out_copy(c):
        return pltpu.make_async_copy(y.at[:, cols(c)], out_hbm.at[:, cols(c)], out_sem.at[c])

    def compute(c, odd, slot, more):
        for r in range(3):
            down_copy(c, slot, r).wait()
        total = None
        for r, (at, depth) in enumerate(COLS):
            part = jnp.dot(
                hidden[:, at : at + depth], ring[slot, :depth, r * NB : (r + 1) * NB], preferred_element_type=jnp.float32
            )
            total = part if total is None else total + part
        term[...] = total
        if more:
            for r in range(3):
                down_copy(c + SLOTS, slot, r).start()
        order = (0, 2, 1, 3) if odd else (0, 1, 2, 3)
        for q, p in enumerate(order):
            own[16 * q : 16 * q + 16, cols(c)] = term[16 * p : 16 * p + 16, :]
            send0[16 * q : 16 * q + 16, cols(c)] = term[64 + 16 * p : 80 + 16 * p, :].astype(jnp.bfloat16)
        c0(c).start()

    def stage1(c, odd):
        c0(c).wait_recv()
        total = own[:, cols(c)] + recv0[:, cols(c)].astype(jnp.float32)
        send1[:, cols(c)] = total[32:].astype(jnp.bfloat16)
        own[0:32, cols(c)] = total[:32]
        c1(c, odd).start()

    def stage2(c, odd):
        c1(c, odd).wait_recv()
        total = own[0:32, cols(c)] + recv1[:, cols(c)].astype(jnp.float32)
        send2[:, cols(c)] = total[16:].astype(jnp.bfloat16)
        own[0:16, cols(c)] = total[:16]
        c2(c, odd).start()

    def stage3(c, odd):
        c2(c, odd).wait_recv()
        total = own[0:16, cols(c)] + recv2[:, cols(c)].astype(jnp.float32)
        y[piece(core, cx, cy), cols(c)] = total.astype(jnp.bfloat16)
        c3(c, odd).start()
        c4(c, odd, False).start()

    def stage4(c, odd):
        c3(c, odd).wait_recv()
        c4(c, odd, True).start()

    def stage5(c, odd):
        c4(c, odd, False).wait_recv()
        c4(c, odd, True).wait_recv()
        c5(c).start()

    def stage6(c, odd):
        c5(c).wait_recv()
        out_copy(c).start()

    stages = tuple(zip(LAGS, (stage1, stage2, stage3, stage4, stage5, stage6)))

    def steps(lo, hi, computing, more):
        def pair(t, _):
            for odd in (0, 1):
                i = 2 * t + odd
                if computing:
                    compute(i, odd, lax.rem(i, SLOTS), more)
                for lag, stage in reversed(stages):
                    c = i - lag
                    c_odd = (odd + lag) % 2
                    if lo - lag >= 0 and hi - 1 - lag < CHUNKS:
                        stage(c, c_odd)
                    else:

                        @pl.when((c >= 0) & (c < CHUNKS))
                        def _(stage=stage, c=c, c_odd=c_odd):
                            stage(c, c_odd)

            return 0

        lax.fori_loop(lo // 2, hi // 2, pair, 0)

    steps(0, CHUNKS - SLOTS, True, True)
    steps(CHUNKS - SLOTS, CHUNKS, True, False)
    steps(CHUNKS, CHUNKS + LAGS[-1] + LAGS[-1] % 2, False, False)

    def drain(t, _):
        for odd in (0, 1):
            c = 2 * t + odd
            c0(c).wait_send()
            c1(c, odd).wait_send()
            c2(c, odd).wait_send()
            c3(c, odd).wait_send()
            c4(c, odd, False).wait_send()
            c4(c, odd, True).wait_send()
            c5(c).wait_send()
            out_copy(c).wait()
        return 0

    lax.fori_loop(0, CHUNKS // 2, drain, 0)


def solution(mesh):
    bf16, f32 = jnp.bfloat16, jnp.float32

    def step(x, w_gate, w_up, w_down):
        dma = pltpu.SemaphoreType.DMA
        return pl.pallas_call(
            kernel,
            out_shape=jax.ShapeDtypeStruct((ROWS, D), bf16),
            in_specs=[pl.BlockSpec(memory_space=pl.ANY)] * 4,
            out_specs=pl.BlockSpec(memory_space=pl.ANY),
            scratch_shapes=[
                pltpu.VMEM((ROWS, D), bf16),
                pltpu.VMEM((ROWS, H), bf16),
                pltpu.VMEM((ROWS, KB), f32),
                pltpu.VMEM((ROWS, KB), f32),
                pltpu.VMEM((SLOTS, KB, KB), bf16),
                pltpu.VMEM((ROWS, NB), f32),
                pltpu.VMEM((64, D), f32),
                pltpu.VMEM((64, D), bf16),
                pltpu.VMEM((64, D), bf16),
                pltpu.VMEM((32, D), bf16),
                pltpu.VMEM((32, D), bf16),
                pltpu.VMEM((16, D), bf16),
                pltpu.VMEM((16, D), bf16),
                pltpu.VMEM((ROWS, D), bf16),
                dma((8,)),
                dma((SLOTS, 3)),
                *[dma((CHUNKS,)) for _ in range(8)],
                dma((CHUNKS, 2)),
                dma((CHUNKS, 2)),
                dma((CHUNKS,)),
                dma((CHUNKS,)),
                dma((CHUNKS,)),
            ],
            compiler_params=pltpu.CompilerParams(
                collective_id=0, has_side_effects=True, vmem_limit_bytes=67_043_328
            ),
            cost_estimate=pl.CostEstimate(
                flops=6 * ROWS * D * H, bytes_accessed=6 * D * H + 4 * ROWS * D, transcendentals=ROWS * H
            ),
        )(x, w_gate, w_up, w_down)

    return jax.shard_map(
        step,
        mesh=mesh,
        in_specs=(P("dp", None), P(None, "tp"), P(None, "tp"), P("tp", None)),
        out_specs=P("dp", None),
        check_vma=False,
    )
```

```python
import functools

import jax
import jax.numpy as jnp
from jax import lax
from jax.experimental import pallas as pl
from jax.experimental.pallas import tpu as pltpu
from jax.sharding import PartitionSpec as P

MESH = pl.DeviceIdType.MESH
ROWS, D, H = 128, 12288, 4224
KB = 1536
COLS = ((0, 1536), (1536, 1536), (3072, 1152))
NB = 512
CHUNKS = D // NB
SLOTS = 8
HALF = SLOTS // 2
LAGS = (2, 6, 10, 14, 18, 20)


def splits(width):
    return [(at, min(512, width - at)) for at in range(0, width, 512)]


def kernel(x_hbm, g_hbm, u_hbm, d_hbm, out_hbm, xv, hidden, acc_g, acc_u, ring, term, own, send0, recv0, send1, recv1,
           send2, recv2, y, x_sem, ring_sem, s0, r0, s1, r1, s2, r2, s3, r3, s4, r4, s5, r5, out_sem):
    me = lax.axis_index("tp")
    core = lax.rem(me, 2)
    cx, cy = me // 4, lax.rem(me // 2, 2)
    code = 4 * core + 2 * cx + cy
    partner = cx * 4 + cy * 2 + (1 - core)
    nbr_x = (1 - cx) * 4 + cy * 2 + core
    nbr_y = cx * 4 + (1 - cy) * 2 + core

    barrier = pltpu.get_barrier_semaphore()
    for peer in (partner, nbr_x, nbr_y):
        pl.semaphore_signal(barrier, inc=1, device_id={"tp": peer}, device_id_type=MESH)

    def x_copy(p):
        ccx, ccy, ccore = cx, cy, core
        if p & 1:
            ccy = 1 - ccy
        if p & 2:
            ccx = 1 - ccx
        if p & 4:
            ccore = 1 - ccore
        row = pl.multiple_of((4 * ccore + 2 * ccx + ccy) * 16, 16)
        return pltpu.make_async_copy(x_hbm.at[pl.ds(row, 16), :], xv.at[pl.ds(16 * p, 16), :], x_sem.at[p])

    def in_copy(w_hbm, nb, kb, slot):
        at, width = COLS[nb]
        return pltpu.make_async_copy(
            w_hbm.at[pl.ds(pl.multiple_of(kb * KB, KB), KB), pl.ds(at, width)],
            ring.at[slot, :, pl.ds(0, width)],
            ring_sem.at[slot, 0],
        )

    def down_copy(j, slot, r):
        at, depth = COLS[r]
        return pltpu.make_async_copy(
            d_hbm.at[pl.ds(at, depth), pl.ds(pl.multiple_of(j * NB, NB), NB)],
            ring.at[slot, pl.ds(0, depth), pl.ds(r * NB, NB)],
            ring_sem.at[slot, r],
        )

    for p in range(8):
        x_copy(p).start()
    for kb in range(HALF):
        in_copy(g_hbm, 0, kb, 2 * kb).start()
        in_copy(u_hbm, 0, kb, 2 * kb + 1).start()
    for p in range(8):
        x_copy(p).wait()

    for nb, (at, width) in enumerate(COLS):
        acc_g[...] = jnp.zeros_like(acc_g)
        acc_u[...] = jnp.zeros_like(acc_u)
        for late in (False, True):

            def body(t, _, nb=nb, width=width, late=late):
                kb = t + HALF if late else t
                xk = xv[:, pl.ds(pl.multiple_of(kb * KB, KB), KB)]
                for which, (w_hbm, acc) in enumerate(((g_hbm, acc_g), (u_hbm, acc_u))):
                    slot = 2 * t + which
                    in_copy(w_hbm, nb, kb, slot).wait()
                    for c, n in splits(width):
                        acc[:, c : c + n] += jnp.dot(xk, ring[slot, :, c : c + n], preferred_element_type=jnp.float32)
                    if not late:
                        in_copy(w_hbm, nb, kb + HALF, slot).start()
                    elif nb + 1 < len(COLS):
                        in_copy(w_hbm, nb + 1, t, slot).start()
                    else:
                        for r in range(3):
                            down_copy(slot, slot, r).start()
                return 0

            lax.fori_loop(0, HALF, body, 0)
        for c, n in splits(width):
            hidden[:, at + c : at + c + n] = (jax.nn.silu(acc_g[:, c : c + n]) * acc_u[:, c : c + n]).astype(jnp.bfloat16)

    pl.semaphore_wait(barrier, 3)

    def rdma(src, dst, send_sem, recv_sem, peer):
        return pltpu.make_async_remote_copy(
            src_ref=src, dst_ref=dst, send_sem=send_sem, recv_sem=recv_sem, device_id={"tp": peer}, device_id_type=MESH
        )

    def cols(c):
        return pl.ds(pl.multiple_of(c * NB, NB), NB)

    def c0(c):
        return rdma(send0.at[:, cols(c)], recv0.at[:, cols(c)], s0.at[c], r0.at[c], partner)

    def c1(c, odd):
        return rdma(send1.at[:, cols(c)], recv1.at[:, cols(c)], s1.at[c], r1.at[c], nbr_y if odd else nbr_x)

    def c2(c, odd):
        return rdma(send2.at[:, cols(c)], recv2.at[:, cols(c)], s2.at[c], r2.at[c], nbr_x if odd else nbr_y)

    def piece(core_, x_, y_):
        return pl.ds(pl.multiple_of((4 * core_ + 2 * x_ + y_) * 16, 16), 16)

    def c3(c, odd):
        at = y.at[piece(core, cx, cy), cols(c)]
        return rdma(at, at, s3.at[c], r3.at[c], nbr_x if odd else nbr_y)

    def c4(c, odd, second):
        if odd:
            at = y.at[piece(core, 1 - cx if second else cx, cy), cols(c)]
        else:
            at = y.at[piece(core, cx, 1 - cy if second else cy), cols(c)]
        return rdma(at, at, s4.at[c, int(second)], r4.at[c, int(second)], nbr_y if odd else nbr_x)

    def c5(c):
        at = y.at[pl.ds(pl.multiple_of(core * 64, 64), 64), cols(c)]
        return rdma(at, at, s5.at[c], r5.at[c], partner)

    def out_copy(c):
        return pltpu.make_async_copy(y.at[:, cols(c)], out_hbm.at[:, cols(c)], out_sem.at[c])

    def compute(c, odd, slot, more):
        for r in range(3):
            down_copy(c, slot, r).wait()
        total = None
        for r, (at, depth) in enumerate(COLS):
            part = jnp.dot(
                hidden[:, at : at + depth], ring[slot, :depth, r * NB : (r + 1) * NB], preferred_element_type=jnp.float32
            )
            total = part if total is None else total + part
        term[...] = total
        if more:
            for r in range(3):
                down_copy(c + SLOTS, slot, r).start()
        order = (0, 2, 1, 3) if odd else (0, 1, 2, 3)
        for q, p in enumerate(order):
            own[16 * q : 16 * q + 16, cols(c)] = term[16 * p : 16 * p + 16, :]
            send0[16 * q : 16 * q + 16, cols(c)] = term[64 + 16 * p : 80 + 16 * p, :].astype(jnp.bfloat16)
        c0(c).start()

    def stage1(c, odd):
        c0(c).wait_recv()
        total = own[:, cols(c)] + recv0[:, cols(c)].astype(jnp.float32)
        send1[:, cols(c)] = total[32:].astype(jnp.bfloat16)
        own[0:32, cols(c)] = total[:32]
        c1(c, odd).start()

    def stage2(c, odd):
        c1(c, odd).wait_recv()
        total = own[0:32, cols(c)] + recv1[:, cols(c)].astype(jnp.float32)
        send2[:, cols(c)] = total[16:].astype(jnp.bfloat16)
        own[0:16, cols(c)] = total[:16]
        c2(c, odd).start()

    def stage3(c, odd):
        c2(c, odd).wait_recv()
        total = own[0:16, cols(c)] + recv2[:, cols(c)].astype(jnp.float32)
        y[piece(core, cx, cy), cols(c)] = total.astype(jnp.bfloat16)
        c3(c, odd).start()
        c4(c, odd, False).start()

    def stage4(c, odd):
        c3(c, odd).wait_recv()
        c4(c, odd, True).start()

    def stage5(c, odd):
        c4(c, odd, False).wait_recv()
        c4(c, odd, True).wait_recv()
        c5(c).start()

    def stage6(c, odd):
        c5(c).wait_recv()
        out_copy(c).start()

    stages = tuple(zip(LAGS, (stage1, stage2, stage3, stage4, stage5, stage6)))

    def steps(lo, hi, computing, more):
        def pair(t, _):
            for odd in (0, 1):
                i = 2 * t + odd
                if computing:
                    compute(i, odd, lax.rem(i, SLOTS), more)
                for lag, stage in reversed(stages):
                    c = i - lag
                    c_odd = (odd + lag) % 2
                    if lo - lag >= 0 and hi - 1 - lag < CHUNKS:
                        stage(c, c_odd)
                    else:

                        @pl.when((c >= 0) & (c < CHUNKS))
                        def _(stage=stage, c=c, c_odd=c_odd):
                            stage(c, c_odd)

            return 0

        lax.fori_loop(lo // 2, hi // 2, pair, 0)

    steps(0, CHUNKS - SLOTS, True, True)
    steps(CHUNKS - SLOTS, CHUNKS, True, False)
    steps(CHUNKS, CHUNKS + LAGS[-1] + LAGS[-1] % 2, False, False)

    def drain(t, _):
        for odd in (0, 1):
            c = 2 * t + odd
            c0(c).wait_send()
            c1(c, odd).wait_send()
            c2(c, odd).wait_send()
            c3(c, odd).wait_send()
            c4(c, odd, False).wait_send()
            c4(c, odd, True).wait_send()
            c5(c).wait_send()
            out_copy(c).wait()
        return 0

    lax.fori_loop(0, CHUNKS // 2, drain, 0)


def solution(mesh):
    bf16, f32 = jnp.bfloat16, jnp.float32

    def step(x, w_gate, w_up, w_down):
        dma = pltpu.SemaphoreType.DMA
        return pl.pallas_call(
            kernel,
            out_shape=jax.ShapeDtypeStruct((ROWS, D), bf16),
            in_specs=[pl.BlockSpec(memory_space=pl.ANY)] * 4,
            out_specs=pl.BlockSpec(memory_space=pl.ANY),
            scratch_shapes=[
                pltpu.VMEM((ROWS, D), bf16),
                pltpu.VMEM((ROWS, H), bf16),
                pltpu.VMEM((ROWS, KB), f32),
                pltpu.VMEM((ROWS, KB), f32),
                pltpu.VMEM((SLOTS, KB, KB), bf16),
                pltpu.VMEM((ROWS, NB), f32),
                pltpu.VMEM((64, D), f32),
                pltpu.VMEM((64, D), bf16),
                pltpu.VMEM((64, D), bf16),
                pltpu.VMEM((32, D), bf16),
                pltpu.VMEM((32, D), bf16),
                pltpu.VMEM((16, D), bf16),
                pltpu.VMEM((16, D), bf16),
                pltpu.VMEM((ROWS, D), bf16),
                dma((8,)),
                dma((SLOTS, 3)),
                *[dma((CHUNKS,)) for _ in range(8)],
                dma((CHUNKS, 2)),
                dma((CHUNKS, 2)),
                dma((CHUNKS,)),
                dma((CHUNKS,)),
                dma((CHUNKS,)),
            ],
            compiler_params=pltpu.CompilerParams(
                collective_id=0, has_side_effects=True, vmem_limit_bytes=67_043_328
            ),
            cost_estimate=pl.CostEstimate(
                flops=6 * ROWS * D * H, bytes_accessed=6 * D * H + 4 * ROWS * D, transcendentals=ROWS * H
            ),
        )(x, w_gate, w_up, w_down)

    return jax.shard_map(
        step,
        mesh=mesh,
        in_specs=(P("dp", None), P(None, "tp"), P(None, "tp"), P("tp", None)),
        out_specs=P("dp", None),
        check_vma=False,
    )
```

```python
import jax
import jax.numpy as jnp
from jax import lax
from jax.experimental import pallas as pl
from jax.experimental.pallas import tpu as pltpu
from jax.sharding import PartitionSpec as P

MESH = pl.DeviceIdType.MESH
ROWS, D, H = 128, 12288, 4224
KB = 1536
COLS = ((0, 1536), (1536, 1536), (3072, 1152))
NB = 512
SLOTS = 8
HALF = SLOTS // 2

CHUNKS = [(512, "2", "2")] * 24
HOP, HOP2, D2D = 2.2, 3.2, 1.1
AXES = {1: ("y",), 2: ("x",), 3: ("x", "y")}


def plan():
    link, rate = 46.65e3, 3.44e6
    free = {"x": 0.0, "y": 0.0}
    arrive, t = [], 1.0
    for w, _, _ in CHUNKS:
        t += 2 * H * w / rate
        arrive.append(t)

    def send(axes, nbytes, now):
        end = max([now] + [free[a] for a in axes]) + nbytes / link
        for a in axes:
            free[a] = end
        return end + (HOP2 if len(axes) == 2 else HOP)

    def many(w, last, now):
        return max([now + D2D] + [send(AXES[p & 3], 32 * w, now) for p in range(1, last) if p & 3])

    order, pending, now, c_next = [], {}, 0.0, 0
    while c_next < len(CHUNKS) or pending:
        ripe = [c for c, v in pending.items() if v[1] <= now]
        if ripe:
            c = min(ripe)
        else:
            options = [(v[1], c) for c, v in pending.items()]
            if c_next < len(CHUNKS):
                options.append((max(arrive[c_next], now), c_next))
            c = min(options)[1]
        w, rs, ag = CHUNKS[c]
        far = AXES[2 if c % 2 == 0 else 1], AXES[1 if c % 2 == 0 else 2]
        if c == c_next:
            c_next += 1
            now = max(now, arrive[c]) + 0.65 * w / 512 + 0.05
            order.append((c, "compute"))
            pending[c] = ("all", many(w, 8, now)) if rs == "d" else ("pair", now + D2D + 128 * w / 650e3)
            continue
        event, at = pending.pop(c)
        now = max(now, at) + 0.08
        order.append((c, event))
        if event == "pair":
            pending[c] = ("first", send(far[0], 64 * w, now)) if rs == "2" else ("three", many(w, 4, now))
        elif event == "first":
            pending[c] = ("second", send(far[1], 32 * w, now))
        elif event in ("second", "three", "all"):
            if ag == "2":
                pending[c] = ("back", send(far[1], 32 * w, now))
                send(far[0], 32 * w, now)
            elif ag == "1":
                pending[c] = ("wide", many(w, 4, now))
            else:
                pending[c] = ("end", many(w, 8, now))
        elif event == "back":
            pending[c] = ("wide", send(far[0], 32 * w, now))
        elif event == "wide":
            pending[c] = ("end", now + D2D + 128 * w / 650e3)
    return order


def copies_of(rs, ag):
    return {"2": 3, "1": 4, "d": 7}[rs] + {"2": 4, "1": 4, "d": 7}[ag]


COPIES = sum(copies_of(rs, ag) for _, rs, ag in CHUNKS)
WIDE = max([w for w, rs, _ in CHUNKS if rs == "d"], default=0)


def blocks():
    out, at = [], 0
    for c, (w, _, _) in enumerate(CHUNKS):
        for b in range(0, w, NB):
            out.append((c, at + b, min(NB, w - b)))
        at += w
    return out


def splits(width):
    return [(at, min(512, width - at)) for at in range(0, width, 512)]


def kernel(x_hbm, g_hbm, u_hbm, d_hbm, y, xv, hidden, acc_g, acc_u, ring, term, own, send_a, recv_a, send_b, recv_b,
           send_d, recv_d, x_sem, ring_sem, send_sem, recv_sem):
    bf16, f32 = jnp.bfloat16, jnp.float32
    me = lax.axis_index("tp")
    place = lax.rem(me, 2), me // 4, lax.rem(me // 2, 2)

    def flip(p):
        return [1 - v if p >> b & 1 else v for v, b in zip(place, (2, 1, 0))]

    def device(p):
        core, x, y_ = flip(p)
        return 4 * x + 2 * y_ + core

    def piece(p):
        core, x, y_ = flip(p)
        return pl.ds(pl.multiple_of((4 * core + 2 * x + y_) * 16, 16), 16)

    barrier = pltpu.get_barrier_semaphore()
    for p in range(1, 8):
        pl.semaphore_signal(barrier, inc=1, device_id={"tp": device(p)}, device_id_type=MESH)

    def x_copy(p):
        return pltpu.make_async_copy(x_hbm.at[piece(p), :], xv.at[pl.ds(16 * p, 16), :], x_sem.at[p])

    def in_copy(w_hbm, nb, kb, slot):
        at, width = COLS[nb]
        return pltpu.make_async_copy(
            w_hbm.at[pl.ds(pl.multiple_of(kb * KB, KB), KB), pl.ds(at, width)],
            ring.at[slot, :, pl.ds(0, width)],
            ring_sem.at[slot, 0],
        )

    tiles = blocks()

    def down_copy(j, r):
        at, depth = COLS[r]
        _, col, w = tiles[j]
        return pltpu.make_async_copy(
            d_hbm.at[pl.ds(at, depth), pl.ds(col, w)],
            ring.at[j % SLOTS, pl.ds(0, depth), pl.ds(r * NB, w)],
            ring_sem.at[j % SLOTS, r],
        )

    for p in range(8):
        x_copy(p).start()
    for kb in range(HALF):
        in_copy(g_hbm, 0, kb, 2 * kb).start()
        in_copy(u_hbm, 0, kb, 2 * kb + 1).start()
    for p in range(8):
        x_copy(p).wait()

    for nb, (at, width) in enumerate(COLS):
        acc_g[...] = jnp.zeros_like(acc_g)
        acc_u[...] = jnp.zeros_like(acc_u)

        def multiply(kb, slot, nb=nb, width=width):
            xk = xv[:, pl.ds(pl.multiple_of(kb * KB, KB), KB)]
            w_hbm, acc = ((g_hbm, acc_g), (u_hbm, acc_u))[slot % 2 if isinstance(slot, int) else slot[1]]
            ref = slot if isinstance(slot, int) else slot[0]
            in_copy(w_hbm, nb, kb, ref).wait()
            for c, n in splits(width):
                acc[:, c : c + n] += jnp.dot(xk, ring[ref, :, c : c + n], preferred_element_type=f32)

        for late in (False, True):
            if late and nb + 1 == len(COLS):
                for t in range(HALF):
                    for which in range(2):
                        multiply(t + HALF, 2 * t + which)
                        for r in range(3):
                            down_copy(2 * t + which, r).start()
                continue

            def body(t, _, nb=nb, late=late):
                for which, w_hbm in enumerate((g_hbm, u_hbm)):
                    slot = 2 * t + which
                    multiply(t + HALF if late else t, (slot, which))
                    if late:
                        in_copy(w_hbm, nb + 1, t, slot).start()
                    else:
                        in_copy(w_hbm, nb, t + HALF, slot).start()
                return 0

            lax.fori_loop(0, HALF, body, 0)
        for c, n in splits(width):
            hidden[:, at + c : at + c + n] = (jax.nn.silu(acc_g[:, c : c + n]) * acc_u[:, c : c + n]).astype(bf16)

    pl.semaphore_wait(barrier, 7)

    started = []

    def send(src, dst, p):
        n = len(started)
        copy = pltpu.make_async_remote_copy(
            src_ref=src, dst_ref=dst, send_sem=send_sem.at[n], recv_sem=recv_sem.at[n],
            device_id={"tp": device(p)}, device_id_type=MESH,
        )
        copy.start()
        started.append(copy)
        return copy

    arriving = {}
    starts = [sum(w for w, _, _ in CHUNKS[:c]) for c in range(len(CHUNKS))]

    def compute(c, cols, axes):
        for j, (chunk, col, w) in enumerate(tiles):
            if chunk != c:
                continue
            total = None
            for r, (at, depth) in enumerate(COLS):
                down_copy(j, r).wait()
            for r, (at, depth) in enumerate(COLS):
                part = jnp.dot(
                    hidden[:, at : at + depth], ring[j % SLOTS, :depth, r * NB : r * NB + w], preferred_element_type=f32
                )
                total = part if total is None else total + part
            term[:, :w] = total
            if j + SLOTS < len(tiles):
                for r in range(3):
                    down_copy(j + SLOTS, r).start()
            here = slice(col, col + w)
            if CHUNKS[c][1] == "d":
                own[:16, here] = term[:16, :w]
                send_d[16:, :w] = term[16:, :w].astype(bf16)
                continue
            for q, p in enumerate((0, axes[1], axes[0], 3)):
                own[16 * q : 16 * q + 16, here] = term[16 * p : 16 * p + 16, :w]
                send_a[16 * q : 16 * q + 16, here] = term[64 + 16 * p : 80 + 16 * p, :w].astype(bf16)
        if CHUNKS[c][1] == "d":
            w = CHUNKS[c][0]
            arriving[c] = [
                send(send_d.at[16 * p : 16 * p + 16, :w], recv_d.at[16 * p : 16 * p + 16, :w], p) for p in (3, 7, 1, 2, 5, 6, 4)
            ]
        else:
            arriving[c] = [send(send_a.at[:, cols], recv_a.at[:, cols], 4)]

    def pair(c, cols, axes):
        total = own[:, cols] + recv_a[:, cols].astype(f32)
        if CHUNKS[c][1] == "2":
            send_b[:32, cols] = total[32:].astype(bf16)
            own[:32, cols] = total[:32]
            arriving[c] = [send(send_b.at[:32, cols], recv_b.at[:32, cols], axes[0])]
        else:
            send_b[:, cols] = total[16:].astype(bf16)
            own[:16, cols] = total[:16]
            arriving[c] = [
                send(send_b.at[16 * q - 16 : 16 * q, cols], recv_b.at[16 * q - 16 : 16 * q, cols], p)
                for q, p in ((3, 3), (1, axes[1]), (2, axes[0]))
            ]

    def first(c, cols, axes):
        total = own[:32, cols] + recv_b[:32, cols].astype(f32)
        send_b[32:, cols] = total[16:].astype(bf16)
        own[:16, cols] = total[:16]
        arriving[c] = [send(send_b.at[32:, cols], recv_b.at[32:, cols], axes[1])]

    def finish(c, cols, axes, total):
        y[piece(0), cols] = total.astype(bf16)
        at = y.at[piece(0), cols]
        ag = CHUNKS[c][2]
        if ag == "2":
            arriving[c] = [send(at, at, axes[1]), send(at, at, axes[0])]
        else:
            arriving[c] = [send(at, at, p) for p in ((3, 1, 2) if ag == "1" else (3, 7, 1, 2, 5, 6, 4))]

    def second(c, cols, axes):
        finish(c, cols, axes, own[:16, cols] + recv_b[32:, cols].astype(f32))

    def three(c, cols, axes):
        total = own[:16, cols]
        for q in range(3):
            total = total + recv_b[16 * q : 16 * q + 16, cols].astype(f32)
        finish(c, cols, axes, total)

    def all_(c, cols, axes):
        w = CHUNKS[c][0]
        total = own[:16, cols]
        for p in range(1, 8):
            total = total + recv_d[16 * p : 16 * p + 16, :w].astype(f32)
        finish(c, cols, axes, total)

    def back(c, cols, axes):
        at = y.at[piece(axes[1]), cols]
        arriving[c] = [arriving[c][1], send(at, at, axes[0])]

    def wide(c, cols, axes):
        at = y.at[pl.ds(pl.multiple_of(place[0] * 64, 64), 64), cols]
        arriving[c] = [send(at, at, 4)]

    events = {"pair": pair, "first": first, "second": second, "three": three, "all": all_, "back": back, "wide": wide}
    for c, event in plan():
        cols = slice(starts[c], starts[c] + CHUNKS[c][0])
        axes = (2, 1) if c % 2 == 0 else (1, 2)
        if event == "compute":
            compute(c, cols, axes)
            continue
        for copy in arriving[c][:1] if event == "back" else arriving[c]:
            copy.wait_recv()
        if event != "end":
            events[event](c, cols, axes)

    for copy in started:
        copy.wait_send()


def solution(mesh):
    bf16, f32 = jnp.bfloat16, jnp.float32

    def step(x, w_gate, w_up, w_down):
        dma = pltpu.SemaphoreType.DMA
        return pl.pallas_call(
            kernel,
            out_shape=pltpu.VMEM((ROWS, D), bf16),
            in_specs=[pl.BlockSpec(memory_space=pl.ANY)] * 4,
            out_specs=pl.BlockSpec(memory_space=pltpu.VMEM),
            scratch_shapes=[
                pltpu.VMEM((ROWS, D), bf16),
                pltpu.VMEM((ROWS, H), bf16),
                pltpu.VMEM((ROWS, KB), f32),
                pltpu.VMEM((ROWS, KB), f32),
                pltpu.VMEM((SLOTS, KB, KB), bf16),
                pltpu.VMEM((ROWS, NB), f32),
                pltpu.VMEM((64, D), f32),
                pltpu.VMEM((64, D), bf16),
                pltpu.VMEM((64, D), bf16),
                pltpu.VMEM((48, D), bf16),
                pltpu.VMEM((48, D), bf16),
                pltpu.VMEM((ROWS, max(WIDE, 128)), bf16),
                pltpu.VMEM((ROWS, max(WIDE, 128)), bf16),
                dma((8,)),
                dma((SLOTS, 3)),
                dma((COPIES,)),
                dma((COPIES,)),
            ],
            compiler_params=pltpu.CompilerParams(
                collective_id=0, has_side_effects=True, vmem_limit_bytes=60 << 20
            ),
            cost_estimate=pl.CostEstimate(
                flops=6 * ROWS * D * H, bytes_accessed=6 * D * H + 4 * ROWS * D, transcendentals=ROWS * H
            ),
        )(x, w_gate, w_up, w_down)

    return jax.shard_map(
        step,
        mesh=mesh,
        in_specs=(P("dp", None), P(None, "tp"), P(None, "tp"), P("tp", None)),
        out_specs=P("dp", None),
        check_vma=False,
    )
```

```python
import jax
import jax.numpy as jnp
from jax import lax
from jax.experimental import pallas as pl
from jax.experimental.pallas import tpu as pltpu
from jax.sharding import PartitionSpec as P

MESH = pl.DeviceIdType.MESH
ROWS, D, H = 128, 12288, 4224
KB = 1536
COLS = ((0, 1536), (1536, 1536), (3072, 1152))
NB = 512
SLOTS = 8
HALF = SLOTS // 2

CHUNKS = [(512, "1", "1")] * 24
HOP, HOP2, D2D = 3.0, 3.9, 1.4
AXES = {1: ("y",), 2: ("x",), 3: ("x", "y")}


def plan():
    link, rate = 46.65e3, 3.44e6
    free = {"x": 0.0, "y": 0.0}
    arrive, t = [], 1.0
    for w, _, _ in CHUNKS:
        t += 2 * H * w / rate
        arrive.append(t)

    def send(axes, nbytes, now):
        end = max([now] + [free[a] for a in axes]) + nbytes / link
        for a in axes:
            free[a] = end
        return end + (HOP2 if len(axes) == 2 else HOP)

    def many(w, last, now):
        return max([now + D2D] + [send(AXES[p & 3], 32 * w, now) for p in range(1, last) if p & 3])

    order, pending, now, c_next = [], {}, 0.0, 0
    while c_next < len(CHUNKS) or pending:
        ripe = [c for c, v in pending.items() if v[1] <= now]
        if ripe:
            c = min(ripe)
        else:
            options = [(v[1], c) for c, v in pending.items()]
            if c_next < len(CHUNKS):
                options.append((max(arrive[c_next], now), c_next))
            c = min(options)[1]
        w, rs, ag = CHUNKS[c]
        far = AXES[2 if c % 2 == 0 else 1], AXES[1 if c % 2 == 0 else 2]
        if c == c_next:
            c_next += 1
            now = max(now, arrive[c]) + 0.65 * w / 512 + 0.05
            order.append((c, "compute"))
            pending[c] = ("all", many(w, 8, now)) if rs == "d" else ("pair", now + D2D + 128 * w / 650e3)
            continue
        event, at = pending.pop(c)
        now = max(now, at) + 0.08
        order.append((c, event))
        if event == "pair":
            pending[c] = ("first", send(far[0], 64 * w, now)) if rs == "2" else ("three", many(w, 4, now))
        elif event == "first":
            pending[c] = ("second", send(far[1], 32 * w, now))
        elif event in ("second", "three", "all"):
            if ag == "2":
                pending[c] = ("back", send(far[1], 32 * w, now))
                send(far[0], 32 * w, now)
            elif ag == "1":
                pending[c] = ("wide", many(w, 4, now))
            else:
                pending[c] = ("end", many(w, 8, now))
        elif event == "back":
            pending[c] = ("wide", send(far[0], 32 * w, now))
        elif event == "wide":
            pending[c] = ("end", now + D2D + 128 * w / 650e3)
    return order


def copies_of(rs, ag):
    return {"2": 3, "1": 4, "d": 7}[rs] + {"2": 4, "1": 4, "d": 7}[ag]


COPIES = sum(copies_of(rs, ag) for _, rs, ag in CHUNKS)
WIDE = max([w for w, rs, _ in CHUNKS if rs == "d"], default=0)


def blocks():
    out, at = [], 0
    for c, (w, _, _) in enumerate(CHUNKS):
        for b in range(0, w, NB):
            out.append((c, at + b, min(NB, w - b)))
        at += w
    return out


def splits(width):
    return [(at, min(512, width - at)) for at in range(0, width, 512)]


def kernel(x_hbm, g_hbm, u_hbm, d_hbm, y, xv, hidden, acc_g, acc_u, ring, term, own, send_a, recv_a, send_b, recv_b,
           send_d, recv_d, x_sem, ring_sem, send_sem, recv_sem):
    bf16, f32 = jnp.bfloat16, jnp.float32
    me = lax.axis_index("tp")
    place = lax.rem(me, 2), me // 4, lax.rem(me // 2, 2)

    def flip(p):
        return [1 - v if p >> b & 1 else v for v, b in zip(place, (2, 1, 0))]

    def device(p):
        core, x, y_ = flip(p)
        return 4 * x + 2 * y_ + core

    def piece(p):
        core, x, y_ = flip(p)
        return pl.ds(pl.multiple_of((4 * core + 2 * x + y_) * 16, 16), 16)

    barrier = pltpu.get_barrier_semaphore()
    for p in range(1, 8):
        pl.semaphore_signal(barrier, inc=1, device_id={"tp": device(p)}, device_id_type=MESH)

    def x_copy(p):
        return pltpu.make_async_copy(x_hbm.at[piece(p), :], xv.at[pl.ds(16 * p, 16), :], x_sem.at[p])

    def in_copy(w_hbm, nb, kb, slot):
        at, width = COLS[nb]
        return pltpu.make_async_copy(
            w_hbm.at[pl.ds(pl.multiple_of(kb * KB, KB), KB), pl.ds(at, width)],
            ring.at[slot, :, pl.ds(0, width)],
            ring_sem.at[slot, 0],
        )

    tiles = blocks()

    def down_copy(j, r):
        at, depth = COLS[r]
        _, col, w = tiles[j]
        return pltpu.make_async_copy(
            d_hbm.at[pl.ds(at, depth), pl.ds(col, w)],
            ring.at[j % SLOTS, pl.ds(0, depth), pl.ds(r * NB, w)],
            ring_sem.at[j % SLOTS, r],
        )

    for p in range(8):
        x_copy(p).start()
    for kb in range(HALF):
        in_copy(g_hbm, 0, kb, 2 * kb).start()
        in_copy(u_hbm, 0, kb, 2 * kb + 1).start()
    for p in range(8):
        x_copy(p).wait()

    for nb, (at, width) in enumerate(COLS):
        acc_g[...] = jnp.zeros_like(acc_g)
        acc_u[...] = jnp.zeros_like(acc_u)

        def multiply(kb, slot, nb=nb, width=width):
            xk = xv[:, pl.ds(pl.multiple_of(kb * KB, KB), KB)]
            w_hbm, acc = ((g_hbm, acc_g), (u_hbm, acc_u))[slot % 2 if isinstance(slot, int) else slot[1]]
            ref = slot if isinstance(slot, int) else slot[0]
            in_copy(w_hbm, nb, kb, ref).wait()
            for c, n in splits(width):
                acc[:, c : c + n] += jnp.dot(xk, ring[ref, :, c : c + n], preferred_element_type=f32)

        for late in (False, True):
            if late and nb + 1 == len(COLS):
                for t in range(HALF):
                    for which in range(2):
                        multiply(t + HALF, 2 * t + which)
                        for r in range(3):
                            down_copy(2 * t + which, r).start()
                continue

            def body(t, _, nb=nb, late=late):
                for which, w_hbm in enumerate((g_hbm, u_hbm)):
                    slot = 2 * t + which
                    multiply(t + HALF if late else t, (slot, which))
                    if late:
                        in_copy(w_hbm, nb + 1, t, slot).start()
                    else:
                        in_copy(w_hbm, nb, t + HALF, slot).start()
                return 0

            lax.fori_loop(0, HALF, body, 0)
        for c, n in splits(width):
            hidden[:, at + c : at + c + n] = (jax.nn.silu(acc_g[:, c : c + n]) * acc_u[:, c : c + n]).astype(bf16)

    pl.semaphore_wait(barrier, 7)

    started = []

    def send(src, dst, p):
        n = len(started)
        copy = pltpu.make_async_remote_copy(
            src_ref=src, dst_ref=dst, send_sem=send_sem.at[n], recv_sem=recv_sem.at[n],
            device_id={"tp": device(p)}, device_id_type=MESH,
        )
        copy.start()
        started.append(copy)
        return copy

    arriving = {}
    starts = [sum(w for w, _, _ in CHUNKS[:c]) for c in range(len(CHUNKS))]

    def compute(c, cols, axes):
        for j, (chunk, col, w) in enumerate(tiles):
            if chunk != c:
                continue
            total = None
            for r, (at, depth) in enumerate(COLS):
                down_copy(j, r).wait()
            for r, (at, depth) in enumerate(COLS):
                part = jnp.dot(
                    hidden[:, at : at + depth], ring[j % SLOTS, :depth, r * NB : r * NB + w], preferred_element_type=f32
                )
                total = part if total is None else total + part
            term[:, :w] = total
            if j + SLOTS < len(tiles):
                for r in range(3):
                    down_copy(j + SLOTS, r).start()
            here = slice(col, col + w)
            if CHUNKS[c][1] == "d":
                own[:16, here] = term[:16, :w]
                send_d[16:, :w] = term[16:, :w].astype(bf16)
                continue
            for q, p in enumerate((0, axes[1], axes[0], 3)):
                own[16 * q : 16 * q + 16, here] = term[16 * p : 16 * p + 16, :w]
                send_a[16 * q : 16 * q + 16, here] = term[64 + 16 * p : 80 + 16 * p, :w].astype(bf16)
        if CHUNKS[c][1] == "d":
            w = CHUNKS[c][0]
            arriving[c] = [
                send(send_d.at[16 * p : 16 * p + 16, :w], recv_d.at[16 * p : 16 * p + 16, :w], p) for p in (3, 7, 1, 2, 5, 6, 4)
            ]
        else:
            arriving[c] = [send(send_a.at[:, cols], recv_a.at[:, cols], 4)]

    def pair(c, cols, axes):
        total = own[:, cols] + recv_a[:, cols].astype(f32)
        if CHUNKS[c][1] == "2":
            send_b[:32, cols] = total[32:].astype(bf16)
            own[:32, cols] = total[:32]
            arriving[c] = [send(send_b.at[:32, cols], recv_b.at[:32, cols], axes[0])]
        else:
            send_b[:, cols] = total[16:].astype(bf16)
            own[:16, cols] = total[:16]
            arriving[c] = [
                send(send_b.at[16 * q - 16 : 16 * q, cols], recv_b.at[16 * q - 16 : 16 * q, cols], p)
                for q, p in ((3, 3), (1, axes[1]), (2, axes[0]))
            ]

    def first(c, cols, axes):
        total = own[:32, cols] + recv_b[:32, cols].astype(f32)
        send_b[32:, cols] = total[16:].astype(bf16)
        own[:16, cols] = total[:16]
        arriving[c] = [send(send_b.at[32:, cols], recv_b.at[32:, cols], axes[1])]

    def finish(c, cols, axes, total):
        y[piece(0), cols] = total.astype(bf16)
        at = y.at[piece(0), cols]
        ag = CHUNKS[c][2]
        if ag == "2":
            arriving[c] = [send(at, at, axes[1]), send(at, at, axes[0])]
        else:
            arriving[c] = [send(at, at, p) for p in ((3, 1, 2) if ag == "1" else (3, 7, 1, 2, 5, 6, 4))]

    def second(c, cols, axes):
        finish(c, cols, axes, own[:16, cols] + recv_b[32:, cols].astype(f32))

    def three(c, cols, axes):
        total = own[:16, cols]
        for q in range(3):
            total = total + recv_b[16 * q : 16 * q + 16, cols].astype(f32)
        finish(c, cols, axes, total)

    def all_(c, cols, axes):
        w = CHUNKS[c][0]
        total = own[:16, cols]
        for p in range(1, 8):
            total = total + recv_d[16 * p : 16 * p + 16, :w].astype(f32)
        finish(c, cols, axes, total)

    def back(c, cols, axes):
        at = y.at[piece(axes[1]), cols]
        arriving[c] = [arriving[c][1], send(at, at, axes[0])]

    def wide(c, cols, axes):
        at = y.at[pl.ds(pl.multiple_of(place[0] * 64, 64), 64), cols]
        arriving[c] = [send(at, at, 4)]

    events = {"pair": pair, "first": first, "second": second, "three": three, "all": all_, "back": back, "wide": wide}
    for c, event in plan():
        cols = slice(starts[c], starts[c] + CHUNKS[c][0])
        axes = (2, 1) if c % 2 == 0 else (1, 2)
        if event == "compute":
            compute(c, cols, axes)
            continue
        for copy in arriving[c][:1] if event == "back" else arriving[c]:
            copy.wait_recv()
        if event != "end":
            events[event](c, cols, axes)

    for copy in started:
        copy.wait_send()


def solution(mesh):
    bf16, f32 = jnp.bfloat16, jnp.float32

    def step(x, w_gate, w_up, w_down):
        dma = pltpu.SemaphoreType.DMA
        return pl.pallas_call(
            kernel,
            out_shape=pltpu.VMEM((ROWS, D), bf16),
            in_specs=[pl.BlockSpec(memory_space=pl.ANY)] * 4,
            out_specs=pl.BlockSpec(memory_space=pltpu.VMEM),
            scratch_shapes=[
                pltpu.VMEM((ROWS, D), bf16),
                pltpu.VMEM((ROWS, H), bf16),
                pltpu.VMEM((ROWS, KB), f32),
                pltpu.VMEM((ROWS, KB), f32),
                pltpu.VMEM((SLOTS, KB, KB), bf16),
                pltpu.VMEM((ROWS, NB), f32),
                pltpu.VMEM((64, D), f32),
                pltpu.VMEM((64, D), bf16),
                pltpu.VMEM((64, D), bf16),
                pltpu.VMEM((48, D), bf16),
                pltpu.VMEM((48, D), bf16),
                pltpu.VMEM((ROWS, max(WIDE, 128)), bf16),
                pltpu.VMEM((ROWS, max(WIDE, 128)), bf16),
                dma((8,)),
                dma((SLOTS, 3)),
                dma((COPIES,)),
                dma((COPIES,)),
            ],
            compiler_params=pltpu.CompilerParams(
                collective_id=0, has_side_effects=True, vmem_limit_bytes=60 << 20
            ),
            cost_estimate=pl.CostEstimate(
                flops=6 * ROWS * D * H, bytes_accessed=6 * D * H + 4 * ROWS * D, transcendentals=ROWS * H
            ),
        )(x, w_gate, w_up, w_down)

    return jax.shard_map(
        step,
        mesh=mesh,
        in_specs=(P("dp", None), P(None, "tp"), P(None, "tp"), P("tp", None)),
        out_specs=P("dp", None),
        check_vma=False,
    )
```

```python
import jax
import jax.numpy as jnp
from jax import lax
from jax.experimental import pallas as pl
from jax.experimental.pallas import tpu as pltpu
from jax.sharding import PartitionSpec as P

MESH = pl.DeviceIdType.MESH
ROWS, D, H = 128, 12288, 4224
KB = 1536
COLS = ((0, 1536), (1536, 1536), (3072, 1152))
NB = 512
SLOTS = 8
HALF = SLOTS // 2

CHUNKS = [(512, "2", "2")] * 20 + [(512, "1", "2")] * 2 + [(512, "1", "1")] * 2
HOP, HOP2, D2D = 2.7, 3.55, 1.6
AXES = {1: ("y",), 2: ("x",), 3: ("x", "y")}


def plan():
    link, rate = 41e3, 3.44e6
    free = {"x": 0.0, "y": 0.0}
    arrive, t = [], 1.0
    for w, _, _ in CHUNKS:
        t += 2 * H * w / rate
        arrive.append(t)

    def send(axes, nbytes, now):
        end = max([now] + [free[a] for a in axes]) + nbytes / link
        for a in axes:
            free[a] = end
        return end + (HOP2 if len(axes) == 2 else HOP)

    def many(w, last, now):
        return max([now + D2D] + [send(AXES[p & 3], 32 * w, now) for p in range(1, last) if p & 3])

    order, pending, now, c_next = [], {}, 0.0, 0
    while c_next < len(CHUNKS) or pending:
        ripe = [c for c, v in pending.items() if v[1] <= now]
        if ripe:
            c = max(ripe)
        else:
            options = [(v[1], c) for c, v in pending.items()]
            if c_next < len(CHUNKS):
                options.append((max(arrive[c_next], now), c_next))
            c = min(options)[1]
        w, rs, ag = CHUNKS[c]
        far = AXES[2 if c % 2 == 0 else 1], AXES[1 if c % 2 == 0 else 2]
        if c == c_next:
            c_next += 1
            now = max(now, arrive[c]) + 0.7 * w / 512 + 0.05
            order.append((c, "compute"))
            pending[c] = ("all", many(w, 8, now)) if rs == "d" else ("pair", now + D2D + 128 * w / 650e3)
            continue
        event, at = pending.pop(c)
        now = max(now, at) + 0.08
        order.append((c, event))
        if event == "pair":
            pending[c] = ("first", send(far[0], 64 * w, now)) if rs == "2" else ("three", many(w, 4, now))
        elif event == "first":
            pending[c] = ("second", send(far[1], 32 * w, now))
        elif event in ("second", "three", "all"):
            if ag == "2":
                pending[c] = ("back", send(far[1], 32 * w, now))
                send(far[0], 32 * w, now)
            elif ag == "1":
                pending[c] = ("wide", many(w, 4, now))
            else:
                pending[c] = ("end", many(w, 8, now))
        elif event == "back":
            pending[c] = ("wide", send(far[0], 32 * w, now))
        elif event == "wide":
            pending[c] = ("end", now + D2D + 128 * w / 650e3)
    return order


def copies_of(rs, ag):
    return {"2": 3, "1": 4, "d": 7}[rs] + {"2": 4, "1": 4, "d": 7}[ag]


COPIES = sum(copies_of(rs, ag) for _, rs, ag in CHUNKS)
WIDE = max([w for w, rs, _ in CHUNKS if rs == "d"], default=0)


def blocks():
    out, at = [], 0
    for c, (w, _, _) in enumerate(CHUNKS):
        for b in range(0, w, NB):
            out.append((c, at + b, min(NB, w - b)))
        at += w
    return out


def splits(width):
    return [(at, min(512, width - at)) for at in range(0, width, 512)]


def kernel(x_hbm, g_hbm, u_hbm, d_hbm, y, xv, hidden, acc_g, acc_u, ring, term, own, send_a, recv_a, send_b, recv_b,
           send_d, recv_d, x_sem, ring_sem, send_sem, recv_sem):
    bf16, f32 = jnp.bfloat16, jnp.float32
    me = lax.axis_index("tp")
    place = lax.rem(me, 2), me // 4, lax.rem(me // 2, 2)

    def flip(p):
        return [1 - v if p >> b & 1 else v for v, b in zip(place, (2, 1, 0))]

    def device(p):
        core, x, y_ = flip(p)
        return 4 * x + 2 * y_ + core

    def piece(p):
        core, x, y_ = flip(p)
        return pl.ds(pl.multiple_of((4 * core + 2 * x + y_) * 16, 16), 16)

    barrier = pltpu.get_barrier_semaphore()
    for p in range(1, 8):
        pl.semaphore_signal(barrier, inc=1, device_id={"tp": device(p)}, device_id_type=MESH)

    def x_copy(p):
        return pltpu.make_async_copy(x_hbm.at[piece(p), :], xv.at[pl.ds(16 * p, 16), :], x_sem.at[p])

    def in_copy(w_hbm, nb, kb, slot):
        at, width = COLS[nb]
        return pltpu.make_async_copy(
            w_hbm.at[pl.ds(pl.multiple_of(kb * KB, KB), KB), pl.ds(at, width)],
            ring.at[slot, :, pl.ds(0, width)],
            ring_sem.at[slot, 0],
        )

    tiles = blocks()

    def down_copy(j, r):
        at, depth = COLS[r]
        _, col, w = tiles[j]
        return pltpu.make_async_copy(
            d_hbm.at[pl.ds(at, depth), pl.ds(col, w)],
            ring.at[j % SLOTS, pl.ds(0, depth), pl.ds(r * NB, w)],
            ring_sem.at[j % SLOTS, r],
        )

    for p in range(8):
        x_copy(p).start()
    for kb in range(HALF):
        in_copy(g_hbm, 0, kb, 2 * kb).start()
        in_copy(u_hbm, 0, kb, 2 * kb + 1).start()
    for p in range(8):
        x_copy(p).wait()

    for nb, (at, width) in enumerate(COLS):
        acc_g[...] = jnp.zeros_like(acc_g)
        acc_u[...] = jnp.zeros_like(acc_u)

        def multiply(kb, slot, nb=nb, width=width):
            xk = xv[:, pl.ds(pl.multiple_of(kb * KB, KB), KB)]
            w_hbm, acc = ((g_hbm, acc_g), (u_hbm, acc_u))[slot % 2 if isinstance(slot, int) else slot[1]]
            ref = slot if isinstance(slot, int) else slot[0]
            in_copy(w_hbm, nb, kb, ref).wait()
            for c, n in splits(width):
                acc[:, c : c + n] += jnp.dot(xk, ring[ref, :, c : c + n], preferred_element_type=f32)

        for late in (False, True):
            if late and nb + 1 == len(COLS):
                for t in range(HALF):
                    for which in range(2):
                        multiply(t + HALF, 2 * t + which)
                        for r in range(3):
                            down_copy(2 * t + which, r).start()
                continue

            def body(t, _, nb=nb, late=late):
                for which, w_hbm in enumerate((g_hbm, u_hbm)):
                    slot = 2 * t + which
                    multiply(t + HALF if late else t, (slot, which))
                    if late:
                        in_copy(w_hbm, nb + 1, t, slot).start()
                    else:
                        in_copy(w_hbm, nb, t + HALF, slot).start()
                return 0

            lax.fori_loop(0, HALF, body, 0)
        for c, n in splits(width):
            hidden[:, at + c : at + c + n] = (jax.nn.silu(acc_g[:, c : c + n]) * acc_u[:, c : c + n]).astype(bf16)

    pl.semaphore_wait(barrier, 7)

    started = []

    def send(src, dst, p):
        n = len(started)
        copy = pltpu.make_async_remote_copy(
            src_ref=src, dst_ref=dst, send_sem=send_sem.at[n], recv_sem=recv_sem.at[n],
            device_id={"tp": device(p)}, device_id_type=MESH,
        )
        copy.start()
        started.append(copy)
        return copy

    arriving = {}
    starts = [sum(w for w, _, _ in CHUNKS[:c]) for c in range(len(CHUNKS))]

    def compute(c, cols, axes):
        for j, (chunk, col, w) in enumerate(tiles):
            if chunk != c:
                continue
            total = None
            for r, (at, depth) in enumerate(COLS):
                down_copy(j, r).wait()
            for r, (at, depth) in enumerate(COLS):
                part = jnp.dot(
                    hidden[:, at : at + depth], ring[j % SLOTS, :depth, r * NB : r * NB + w], preferred_element_type=f32
                )
                total = part if total is None else total + part
            term[:, :w] = total
            if j + SLOTS < len(tiles):
                for r in range(3):
                    down_copy(j + SLOTS, r).start()
            here = slice(col, col + w)
            if CHUNKS[c][1] == "d":
                own[:16, here] = term[:16, :w]
                send_d[16:, :w] = term[16:, :w].astype(bf16)
                continue
            for q, p in enumerate((0, axes[1], axes[0], 3)):
                own[16 * q : 16 * q + 16, here] = term[16 * p : 16 * p + 16, :w]
                send_a[16 * q : 16 * q + 16, here] = term[64 + 16 * p : 80 + 16 * p, :w].astype(bf16)
        if CHUNKS[c][1] == "d":
            w = CHUNKS[c][0]
            arriving[c] = [
                send(send_d.at[16 * p : 16 * p + 16, :w], recv_d.at[16 * p : 16 * p + 16, :w], p) for p in (3, 7, 1, 2, 5, 6, 4)
            ]
        else:
            arriving[c] = [send(send_a.at[:, cols], recv_a.at[:, cols], 4)]

    def pair(c, cols, axes):
        total = own[:, cols] + recv_a[:, cols].astype(f32)
        if CHUNKS[c][1] == "2":
            send_b[:32, cols] = total[32:].astype(bf16)
            own[:32, cols] = total[:32]
            arriving[c] = [send(send_b.at[:32, cols], recv_b.at[:32, cols], axes[0])]
        else:
            send_b[:, cols] = total[16:].astype(bf16)
            own[:16, cols] = total[:16]
            arriving[c] = [
                send(send_b.at[16 * q - 16 : 16 * q, cols], recv_b.at[16 * q - 16 : 16 * q, cols], p)
                for q, p in ((3, 3), (1, axes[1]), (2, axes[0]))
            ]

    def first(c, cols, axes):
        total = own[:32, cols] + recv_b[:32, cols].astype(f32)
        send_b[32:, cols] = total[16:].astype(bf16)
        own[:16, cols] = total[:16]
        arriving[c] = [send(send_b.at[32:, cols], recv_b.at[32:, cols], axes[1])]

    def finish(c, cols, axes, total):
        y[piece(0), cols] = total.astype(bf16)
        at = y.at[piece(0), cols]
        ag = CHUNKS[c][2]
        if ag == "2":
            arriving[c] = [send(at, at, axes[1]), send(at, at, axes[0])]
        else:
            arriving[c] = [send(at, at, p) for p in ((3, 1, 2) if ag == "1" else (3, 7, 1, 2, 5, 6, 4))]

    def second(c, cols, axes):
        finish(c, cols, axes, own[:16, cols] + recv_b[32:, cols].astype(f32))

    def three(c, cols, axes):
        total = own[:16, cols]
        for q in range(3):
            total = total + recv_b[16 * q : 16 * q + 16, cols].astype(f32)
        finish(c, cols, axes, total)

    def all_(c, cols, axes):
        w = CHUNKS[c][0]
        total = own[:16, cols]
        for p in range(1, 8):
            total = total + recv_d[16 * p : 16 * p + 16, :w].astype(f32)
        finish(c, cols, axes, total)

    def back(c, cols, axes):
        at = y.at[piece(axes[1]), cols]
        arriving[c] = [arriving[c][1], send(at, at, axes[0])]

    def wide(c, cols, axes):
        at = y.at[pl.ds(pl.multiple_of(place[0] * 64, 64), 64), cols]
        arriving[c] = [send(at, at, 4)]

    events = {"pair": pair, "first": first, "second": second, "three": three, "all": all_, "back": back, "wide": wide}
    for c, event in plan():
        cols = slice(starts[c], starts[c] + CHUNKS[c][0])
        axes = (2, 1) if c % 2 == 0 else (1, 2)
        if event == "compute":
            compute(c, cols, axes)
            continue
        for copy in arriving[c][:1] if event == "back" else arriving[c]:
            copy.wait_recv()
        if event != "end":
            events[event](c, cols, axes)

    for copy in started:
        copy.wait_send()


def solution(mesh):
    bf16, f32 = jnp.bfloat16, jnp.float32

    def step(x, w_gate, w_up, w_down):
        dma = pltpu.SemaphoreType.DMA
        return pl.pallas_call(
            kernel,
            out_shape=pltpu.VMEM((ROWS, D), bf16),
            in_specs=[pl.BlockSpec(memory_space=pl.ANY)] * 4,
            out_specs=pl.BlockSpec(memory_space=pltpu.VMEM),
            scratch_shapes=[
                pltpu.VMEM((ROWS, D), bf16),
                pltpu.VMEM((ROWS, H), bf16),
                pltpu.VMEM((ROWS, KB), f32),
                pltpu.VMEM((ROWS, KB), f32),
                pltpu.VMEM((SLOTS, KB, KB), bf16),
                pltpu.VMEM((ROWS, NB), f32),
                pltpu.VMEM((64, D), f32),
                pltpu.VMEM((64, D), bf16),
                pltpu.VMEM((64, D), bf16),
                pltpu.VMEM((48, D), bf16),
                pltpu.VMEM((48, D), bf16),
                pltpu.VMEM((ROWS, max(WIDE, 128)), bf16),
                pltpu.VMEM((ROWS, max(WIDE, 128)), bf16),
                dma((8,)),
                dma((SLOTS, 3)),
                dma((COPIES,)),
                dma((COPIES,)),
            ],
            compiler_params=pltpu.CompilerParams(
                collective_id=0, has_side_effects=True, vmem_limit_bytes=60 << 20
            ),
            cost_estimate=pl.CostEstimate(
                flops=6 * ROWS * D * H, bytes_accessed=6 * D * H + 4 * ROWS * D, transcendentals=ROWS * H
            ),
        )(x, w_gate, w_up, w_down)

    return jax.shard_map(
        step,
        mesh=mesh,
        in_specs=(P("dp", None), P(None, "tp"), P(None, "tp"), P("tp", None)),
        out_specs=P("dp", None),
        check_vma=False,
    )
```

```python
import jax
import jax.numpy as jnp
from jax import lax
from jax.experimental import pallas as pl
from jax.experimental.pallas import tpu as pltpu
from jax.sharding import PartitionSpec as P

MESH = pl.DeviceIdType.MESH
ROWS, D, H = 128, 12288, 4224
KB = 1536
COLS = ((0, 1536), (1536, 1536), (3072, 1152))
NB = 512
CHUNKS = D // NB
TWO = 20
LAGS_TWO = (1, 4, 7, 10, 13, 15)
LAGS_ONE = (1, 5, 9, 11)
SLOTS = 8
WIDTH = 1408
KS, TILES = D // KB, D // KB * (H // WIDTH)

def splits(width):
    return [(at, min(512, width - at)) for at in range(0, width, 512)]


def kernel(x_hbm, g_hbm, u_hbm, d_hbm, y, xv, hidden, acc_g, acc_u, ring, term, own, send_a, recv_a, send_b, recv_b,
           x_sem, ring_sem, send_sem, recv_sem):
    bf16, f32 = jnp.bfloat16, jnp.float32
    me = lax.axis_index("tp")
    place = lax.rem(me, 2), me // 4, lax.rem(me // 2, 2)

    def flip(p):
        return [1 - v if p >> b & 1 else v for v, b in zip(place, (2, 1, 0))]

    def device(p):
        core, x, y_ = flip(p)
        return 4 * x + 2 * y_ + core

    def piece(p):
        core, x, y_ = flip(p)
        return pl.ds(pl.multiple_of((4 * core + 2 * x + y_) * 16, 16), 16)

    barrier = pltpu.get_barrier_semaphore()
    for p in range(1, 8):
        pl.semaphore_signal(barrier, inc=1, device_id={"tp": device(p)}, device_id_type=MESH)

    def x_copy(p):
        return pltpu.make_async_copy(x_hbm.at[piece(p), :], xv.at[pl.ds(16 * p, 16), :], x_sem.at[p])

    def in_copy(w_hbm, t, slot):
        row = pl.multiple_of(lax.rem(t, KS) * KB, KB)
        col = pl.multiple_of(t // KS * WIDTH, 128)
        return pltpu.make_async_copy(
            w_hbm.at[pl.ds(row, KB), pl.ds(col, WIDTH)], ring.at[slot, :, pl.ds(0, WIDTH)], ring_sem.at[slot, 0]
        )

    def cols(c):
        return pl.ds(pl.multiple_of(c * NB, NB), NB)

    def down_copy(c, slot, r):
        at, depth = COLS[r]
        return pltpu.make_async_copy(
            d_hbm.at[pl.ds(at, depth), cols(c)], ring.at[slot, pl.ds(0, depth), pl.ds(r * NB, NB)], ring_sem.at[slot, r]
        )

    for p in range(8):
        x_copy(p).start()
    for t in range(SLOTS // 2):
        in_copy(g_hbm, t, 2 * t).start()
        in_copy(u_hbm, t, 2 * t + 1).start()
    for p in range(8):
        x_copy(p).wait()

    def project(t, _):
        kb = lax.rem(t, KS)

        @pl.when(kb == 0)
        def _():
            acc_g[...] = jnp.zeros_like(acc_g)
            acc_u[...] = jnp.zeros_like(acc_u)

        xk = xv[:, pl.ds(pl.multiple_of(kb * KB, KB), KB)]
        for which, (w_hbm, acc) in enumerate(((g_hbm, acc_g), (u_hbm, acc_u))):
            slot = 2 * lax.rem(t, SLOTS // 2) + which
            in_copy(w_hbm, t, slot).wait()
            for c, n in splits(WIDTH):
                acc[:, c : c + n] += jnp.dot(xk, ring[slot, :, c : c + n], preferred_element_type=f32)

            @pl.when(t < TILES - SLOTS // 2)
            def _(w_hbm=w_hbm, slot=slot):
                in_copy(w_hbm, t + SLOTS // 2, slot).start()

            @pl.when(t >= TILES - SLOTS // 2)
            def _(slot=slot):
                for r in range(3):
                    down_copy(slot, slot, r).start()

        @pl.when(kb == KS - 1)
        def _():
            for c, n in splits(WIDTH):
                at = pl.ds(pl.multiple_of(t // KS * WIDTH + c, 128), n)
                hidden[:, at] = (jax.nn.silu(acc_g[:, c : c + n]) * acc_u[:, c : c + n]).astype(bf16)

        return 0

    lax.fori_loop(0, TILES, project, 0)

    pl.semaphore_wait(barrier, 7)

    def copy(k, src, dst, c, p):
        return pltpu.make_async_remote_copy(
            src_ref=src, dst_ref=dst, send_sem=send_sem.at[k, c], recv_sem=recv_sem.at[k, c],
            device_id={"tp": device(p)}, device_id_type=MESH,
        )

    def axes_of(odd):
        return (1, 2) if odd else (2, 1)

    def pair_copy(c):
        return copy(0, send_a.at[:, cols(c)], recv_a.at[:, cols(c)], c, 4)

    def sum_copy(c, k, rows, p):
        return copy(k, send_b.at[rows, cols(c)], recv_b.at[rows, cols(c)], c, p)

    def first_copy(c, odd):
        return sum_copy(c, 1, pl.ds(0, 32), axes_of(odd)[0])

    def second_copy(c, odd):
        return sum_copy(c, 2, pl.ds(32, 16), axes_of(odd)[1])

    def three_copies(c, odd):
        a, b = axes_of(odd)
        return [sum_copy(c, k, pl.ds(16 * k - 16, 16), p) for k, p in ((3, 3), (1, b), (2, a))]

    def out_copy(c, k, owner, p):
        at = y.at[piece(owner), cols(c)]
        return copy(k, at, at, c, p)

    def two_copies(c, odd):
        a, b = axes_of(odd)
        return [out_copy(c, 4, 0, b), out_copy(c, 5, 0, a)]

    def back_copy(c, odd):
        a, b = axes_of(odd)
        return out_copy(c, 7, b, a)

    def all_copies(c):
        return [out_copy(c, 7, 0, 3), out_copy(c, 4, 0, 1), out_copy(c, 5, 0, 2)]

    def wide_copy(c):
        at = y.at[pl.ds(pl.multiple_of(place[0] * 64, 64), 64), cols(c)]
        return copy(6, at, at, c, 4)

    def compute(c, odd):
        slot = lax.rem(c, SLOTS)
        for r in range(3):
            down_copy(c, slot, r).wait()
        total = None
        for r, (at, depth) in enumerate(COLS):
            part = jnp.dot(
                hidden[:, at : at + depth], ring[slot, :depth, r * NB : (r + 1) * NB], preferred_element_type=f32
            )
            total = part if total is None else total + part
        term[...] = total

        @pl.when(c + SLOTS < CHUNKS)
        def _():
            for r in range(3):
                down_copy(c + SLOTS, slot, r).start()

        a, b = axes_of(odd)
        for q, p in enumerate((0, b, a, 3)):
            own[16 * q : 16 * q + 16, cols(c)] = term[16 * p : 16 * p + 16, :]
            send_a[16 * q : 16 * q + 16, cols(c)] = term[64 + 16 * p : 80 + 16 * p, :].astype(bf16)
        pair_copy(c).start()

    def start(copies):
        for one in copies:
            one.start()

    def pair_two(c, odd):
        pair_copy(c).wait_recv()
        total = own[:, cols(c)] + recv_a[:, cols(c)].astype(f32)
        send_b[:32, cols(c)] = total[32:].astype(bf16)
        own[:32, cols(c)] = total[:32]
        first_copy(c, odd).start()

    def first(c, odd):
        first_copy(c, odd).wait_recv()
        total = own[:32, cols(c)] + recv_b[:32, cols(c)].astype(f32)
        send_b[32:, cols(c)] = total[16:].astype(bf16)
        own[:16, cols(c)] = total[:16]
        second_copy(c, odd).start()

    def second(c, odd):
        second_copy(c, odd).wait_recv()
        y[piece(0), cols(c)] = (own[:16, cols(c)] + recv_b[32:, cols(c)].astype(f32)).astype(bf16)
        start(two_copies(c, odd))

    def back(c, odd):
        two_copies(c, odd)[0].wait_recv()
        back_copy(c, odd).start()

    def wide_two(c, odd):
        two_copies(c, odd)[1].wait_recv()
        back_copy(c, odd).wait_recv()
        wide_copy(c).start()

    def pair_one(c, odd):
        pair_copy(c).wait_recv()
        total = own[:, cols(c)] + recv_a[:, cols(c)].astype(f32)
        send_b[:, cols(c)] = total[16:].astype(bf16)
        own[:16, cols(c)] = total[:16]
        start(three_copies(c, odd))

    def three(c, odd):
        for one in three_copies(c, odd):
            one.wait_recv()
        total = own[:16, cols(c)]
        for q in range(3):
            total = total + recv_b[16 * q : 16 * q + 16, cols(c)].astype(f32)
        y[piece(0), cols(c)] = total.astype(bf16)
        start(all_copies(c))

    def wide_one(c, odd):
        for one in all_copies(c):
            one.wait_recv()
        wide_copy(c).start()

    def end(c, odd):
        wide_copy(c).wait_recv()

    stages = [(lag, f, 0, TWO) for lag, f in zip(LAGS_TWO, (pair_two, first, second, back, wide_two, end))]
    stages += [(lag, f, TWO, CHUNKS) for lag, f in zip(LAGS_ONE, (pair_one, three, wide_one, end))]
    stages.sort(key=lambda s: (s[0], -s[2]))

    def steps(lo, hi):
        def two_steps(t, _):
            for odd in (0, 1):
                i = 2 * t + odd
                if lo < CHUNKS:
                    compute(i, odd)
                for lag, stage, begin, stop in stages:
                    c, c_odd = i - lag, (odd + lag) % 2
                    if hi - 1 - lag < begin or lo - lag >= stop:
                        continue
                    if lo - lag >= begin and hi - 1 - lag < stop:
                        stage(c, c_odd)
                        continue

                    @pl.when((c >= begin) & (c < stop))
                    def _(stage=stage, c=c, c_odd=c_odd):
                        stage(c, c_odd)

            return 0

        lax.fori_loop(lo // 2, hi // 2, two_steps, 0)

    last = max(TWO - 1 + LAGS_TWO[-1] if TWO else 0, CHUNKS - 1 + LAGS_ONE[-1] if TWO < CHUNKS else 0) + 1
    steps(0, CHUNKS)
    steps(CHUNKS, last + last % 2)

    def drain(t, _):
        for odd in (0, 1):
            c = 2 * t + odd
            pair_copy(c).wait_send()
            wide_copy(c).wait_send()

            @pl.when(c < TWO)
            def _(c=c, odd=odd):
                for one in (first_copy(c, odd), second_copy(c, odd), *two_copies(c, odd), back_copy(c, odd)):
                    one.wait_send()

            @pl.when(c >= TWO)
            def _(c=c, odd=odd):
                for one in three_copies(c, odd) + all_copies(c):
                    one.wait_send()

        return 0

    lax.fori_loop(0, CHUNKS // 2, drain, 0)


def solution(mesh):
    bf16, f32 = jnp.bfloat16, jnp.float32

    def step(x, w_gate, w_up, w_down):
        dma = pltpu.SemaphoreType.DMA
        return pl.pallas_call(
            kernel,
            out_shape=pltpu.VMEM((ROWS, D), bf16),
            in_specs=[pl.BlockSpec(memory_space=pl.ANY)] * 4,
            out_specs=pl.BlockSpec(memory_space=pltpu.VMEM),
            scratch_shapes=[
                pltpu.VMEM((ROWS, D), bf16),
                pltpu.VMEM((ROWS, H), bf16),
                pltpu.VMEM((ROWS, WIDTH), f32),
                pltpu.VMEM((ROWS, WIDTH), f32),
                pltpu.VMEM((SLOTS, KB, KB), bf16),
                pltpu.VMEM((ROWS, NB), f32),
                pltpu.VMEM((64, D), f32),
                pltpu.VMEM((64, D), bf16),
                pltpu.VMEM((64, D), bf16),
                pltpu.VMEM((48, D), bf16),
                pltpu.VMEM((48, D), bf16),
                dma((8,)),
                dma((SLOTS, 3)),
                dma((8, CHUNKS)),
                dma((8, CHUNKS)),
            ],
            compiler_params=pltpu.CompilerParams(
                collective_id=0, has_side_effects=True, vmem_limit_bytes=60 << 20
            ),
            cost_estimate=pl.CostEstimate(
                flops=6 * ROWS * D * H, bytes_accessed=6 * D * H + 4 * ROWS * D, transcendentals=ROWS * H
            ),
        )(x, w_gate, w_up, w_down)

    return jax.shard_map(
        step,
        mesh=mesh,
        in_specs=(P("dp", None), P(None, "tp"), P(None, "tp"), P("tp", None)),
        out_specs=P("dp", None),
        check_vma=False,
    )
```

```python
import jax
import jax.numpy as jnp
from jax import lax
from jax.experimental import pallas as pl
from jax.experimental.pallas import tpu as pltpu
from jax.sharding import PartitionSpec as P

MESH = pl.DeviceIdType.MESH
ROWS, D, H = 128, 12288, 4224
KB = 1536
COLS = ((0, 1536), (1536, 1536), (3072, 1152))
NB = 512
CHUNKS = D // NB
TWO = 20
LAGS_TWO = (1, 4, 7, 10, 13, 15)
LAGS_ONE = (1, 5, 9, 11)
SLOTS = 4
WIDTH = 1408
KS, TILES = D // KB, D // KB * (H // WIDTH)

def splits(width):
    return [(at, min(512, width - at)) for at in range(0, width, 512)]


def kernel(x_hbm, g_hbm, u_hbm, d_hbm, y, xv, hidden, acc_g, acc_u, ring, term, own, send_a, recv_a, send_b, recv_b,
           x_sem, ring_sem, send_sem, recv_sem):
    bf16, f32 = jnp.bfloat16, jnp.float32
    me = lax.axis_index("tp")
    place = lax.rem(me, 2), me // 4, lax.rem(me // 2, 2)

    def flip(p):
        return [1 - v if p >> b & 1 else v for v, b in zip(place, (2, 1, 0))]

    def device(p):
        core, x, y_ = flip(p)
        return 4 * x + 2 * y_ + core

    def piece(p):
        core, x, y_ = flip(p)
        return pl.ds(pl.multiple_of((4 * core + 2 * x + y_) * 16, 16), 16)

    barrier = pltpu.get_barrier_semaphore()
    for p in range(1, 8):
        pl.semaphore_signal(barrier, inc=1, device_id={"tp": device(p)}, device_id_type=MESH)

    def x_copy(p):
        return pltpu.make_async_copy(x_hbm.at[piece(p), :], xv.at[pl.ds(16 * p, 16), :], x_sem.at[p])

    def in_copy(w_hbm, t, slot):
        row = pl.multiple_of(lax.rem(t, KS) * KB, KB)
        col = pl.multiple_of(t // KS * WIDTH, 128)
        return pltpu.make_async_copy(
            w_hbm.at[pl.ds(row, KB), pl.ds(col, WIDTH)], ring.at[slot, :, pl.ds(0, WIDTH)], ring_sem.at[slot, 0]
        )

    def cols(c):
        return pl.ds(pl.multiple_of(c * NB, NB), NB)

    def down_copy(c, slot, r):
        at, depth = COLS[r]
        return pltpu.make_async_copy(
            d_hbm.at[pl.ds(at, depth), cols(c)], ring.at[slot, pl.ds(0, depth), pl.ds(r * NB, NB)], ring_sem.at[slot, r]
        )

    for p in range(8):
        x_copy(p).start()
    for t in range(SLOTS // 2):
        in_copy(g_hbm, t, 2 * t).start()
        in_copy(u_hbm, t, 2 * t + 1).start()
    for p in range(8):
        x_copy(p).wait()

    def project(t, _):
        kb = lax.rem(t, KS)

        @pl.when(kb == 0)
        def _():
            acc_g[...] = jnp.zeros_like(acc_g)
            acc_u[...] = jnp.zeros_like(acc_u)

        xk = xv[:, pl.ds(pl.multiple_of(kb * KB, KB), KB)]
        for which, (w_hbm, acc) in enumerate(((g_hbm, acc_g), (u_hbm, acc_u))):
            slot = 2 * lax.rem(t, SLOTS // 2) + which
            in_copy(w_hbm, t, slot).wait()
            for c, n in splits(WIDTH):
                acc[:, c : c + n] += jnp.dot(xk, ring[slot, :, c : c + n], preferred_element_type=f32)

            @pl.when(t < TILES - SLOTS // 2)
            def _(w_hbm=w_hbm, slot=slot):
                in_copy(w_hbm, t + SLOTS // 2, slot).start()

            @pl.when(t >= TILES - SLOTS // 2)
            def _(slot=slot):
                for r in range(3):
                    down_copy(slot, slot, r).start()

        @pl.when(kb == KS - 1)
        def _():
            for c, n in splits(WIDTH):
                at = pl.ds(pl.multiple_of(t // KS * WIDTH + c, 128), n)
                hidden[:, at] = (jax.nn.silu(acc_g[:, c : c + n]) * acc_u[:, c : c + n]).astype(bf16)

        return 0

    lax.fori_loop(0, TILES, project, 0)

    pl.semaphore_wait(barrier, 7)

    def copy(k, src, dst, c, p):
        return pltpu.make_async_remote_copy(
            src_ref=src, dst_ref=dst, send_sem=send_sem.at[k, c], recv_sem=recv_sem.at[k, c],
            device_id={"tp": device(p)}, device_id_type=MESH,
        )

    def axes_of(odd):
        return (1, 2) if odd else (2, 1)

    def pair_copy(c):
        return copy(0, send_a.at[:, cols(c)], recv_a.at[:, cols(c)], c, 4)

    def sum_copy(c, k, rows, p):
        return copy(k, send_b.at[rows, cols(c)], recv_b.at[rows, cols(c)], c, p)

    def first_copy(c, odd):
        return sum_copy(c, 1, pl.ds(0, 32), axes_of(odd)[0])

    def second_copy(c, odd):
        return sum_copy(c, 2, pl.ds(32, 16), axes_of(odd)[1])

    def three_copies(c, odd):
        a, b = axes_of(odd)
        return [sum_copy(c, k, pl.ds(16 * k - 16, 16), p) for k, p in ((3, 3), (1, b), (2, a))]

    def out_copy(c, k, owner, p):
        at = y.at[piece(owner), cols(c)]
        return copy(k, at, at, c, p)

    def two_copies(c, odd):
        a, b = axes_of(odd)
        return [out_copy(c, 4, 0, b), out_copy(c, 5, 0, a)]

    def back_copy(c, odd):
        a, b = axes_of(odd)
        return out_copy(c, 7, b, a)

    def all_copies(c):
        return [out_copy(c, 7, 0, 3), out_copy(c, 4, 0, 1), out_copy(c, 5, 0, 2)]

    def wide_copy(c):
        at = y.at[pl.ds(pl.multiple_of(place[0] * 64, 64), 64), cols(c)]
        return copy(6, at, at, c, 4)

    def compute(c, odd):
        slot = lax.rem(c, SLOTS)
        for r in range(3):
            down_copy(c, slot, r).wait()
        total = None
        for r, (at, depth) in enumerate(COLS):
            part = jnp.dot(
                hidden[:, at : at + depth], ring[slot, :depth, r * NB : (r + 1) * NB], preferred_element_type=f32
            )
            total = part if total is None else total + part
        term[...] = total

        @pl.when(c + SLOTS < CHUNKS)
        def _():
            for r in range(3):
                down_copy(c + SLOTS, slot, r).start()

        a, b = axes_of(odd)
        for q, p in enumerate((0, b, a, 3)):
            own[16 * q : 16 * q + 16, cols(c)] = term[16 * p : 16 * p + 16, :]
            send_a[16 * q : 16 * q + 16, cols(c)] = term[64 + 16 * p : 80 + 16 * p, :].astype(bf16)
        pair_copy(c).start()

    def start(copies):
        for one in copies:
            one.start()

    def pair_two(c, odd):
        pair_copy(c).wait_recv()
        total = own[:, cols(c)] + recv_a[:, cols(c)].astype(f32)
        send_b[:32, cols(c)] = total[32:].astype(bf16)
        own[:32, cols(c)] = total[:32]
        first_copy(c, odd).start()

    def first(c, odd):
        first_copy(c, odd).wait_recv()
        total = own[:32, cols(c)] + recv_b[:32, cols(c)].astype(f32)
        send_b[32:, cols(c)] = total[16:].astype(bf16)
        own[:16, cols(c)] = total[:16]
        second_copy(c, odd).start()

    def second(c, odd):
        second_copy(c, odd).wait_recv()
        y[piece(0), cols(c)] = (own[:16, cols(c)] + recv_b[32:, cols(c)].astype(f32)).astype(bf16)
        start(two_copies(c, odd))

    def back(c, odd):
        two_copies(c, odd)[0].wait_recv()
        back_copy(c, odd).start()

    def wide_two(c, odd):
        two_copies(c, odd)[1].wait_recv()
        back_copy(c, odd).wait_recv()
        wide_copy(c).start()

    def pair_one(c, odd):
        pair_copy(c).wait_recv()
        total = own[:, cols(c)] + recv_a[:, cols(c)].astype(f32)
        send_b[:, cols(c)] = total[16:].astype(bf16)
        own[:16, cols(c)] = total[:16]
        start(three_copies(c, odd))

    def three(c, odd):
        for one in three_copies(c, odd):
            one.wait_recv()
        total = own[:16, cols(c)]
        for q in range(3):
            total = total + recv_b[16 * q : 16 * q + 16, cols(c)].astype(f32)
        y[piece(0), cols(c)] = total.astype(bf16)
        start(all_copies(c))

    def wide_one(c, odd):
        for one in all_copies(c):
            one.wait_recv()
        wide_copy(c).start()

    def end(c, odd):
        wide_copy(c).wait_recv()

    stages = [(lag, f, 0, TWO) for lag, f in zip(LAGS_TWO, (pair_two, first, second, back, wide_two, end))]
    stages += [(lag, f, TWO, CHUNKS) for lag, f in zip(LAGS_ONE, (pair_one, three, wide_one, end))]
    stages.sort(key=lambda s: (s[0], -s[2]))

    def steps(lo, hi):
        def two_steps(t, _):
            for odd in (0, 1):
                i = 2 * t + odd
                if lo < CHUNKS:
                    compute(i, odd)
                for lag, stage, begin, stop in stages:
                    c, c_odd = i - lag, (odd + lag) % 2
                    if hi - 1 - lag < begin or lo - lag >= stop:
                        continue
                    if lo - lag >= begin and hi - 1 - lag < stop:
                        stage(c, c_odd)
                        continue

                    @pl.when((c >= begin) & (c < stop))
                    def _(stage=stage, c=c, c_odd=c_odd):
                        stage(c, c_odd)

            return 0

        lax.fori_loop(lo // 2, hi // 2, two_steps, 0)

    last = max(TWO - 1 + LAGS_TWO[-1] if TWO else 0, CHUNKS - 1 + LAGS_ONE[-1] if TWO < CHUNKS else 0) + 1
    steps(0, CHUNKS)
    steps(CHUNKS, last + last % 2)

    def drain(t, _):
        for odd in (0, 1):
            c = 2 * t + odd
            pair_copy(c).wait_send()
            wide_copy(c).wait_send()

            @pl.when(c < TWO)
            def _(c=c, odd=odd):
                for one in (first_copy(c, odd), second_copy(c, odd), *two_copies(c, odd), back_copy(c, odd)):
                    one.wait_send()

            @pl.when(c >= TWO)
            def _(c=c, odd=odd):
                for one in three_copies(c, odd) + all_copies(c):
                    one.wait_send()

        return 0

    lax.fori_loop(0, CHUNKS // 2, drain, 0)


def solution(mesh):
    bf16, f32 = jnp.bfloat16, jnp.float32

    def step(x, w_gate, w_up, w_down):
        dma = pltpu.SemaphoreType.DMA
        return pl.pallas_call(
            kernel,
            out_shape=pltpu.VMEM((ROWS, D), bf16),
            in_specs=[pl.BlockSpec(memory_space=pl.ANY)] * 4,
            out_specs=pl.BlockSpec(memory_space=pltpu.VMEM),
            scratch_shapes=[
                pltpu.VMEM((ROWS, D), bf16),
                pltpu.VMEM((ROWS, H), bf16),
                pltpu.VMEM((ROWS, WIDTH), f32),
                pltpu.VMEM((ROWS, WIDTH), f32),
                pltpu.VMEM((SLOTS, KB, KB), bf16),
                pltpu.VMEM((ROWS, NB), f32),
                pltpu.VMEM((64, D), f32),
                pltpu.VMEM((64, D), bf16),
                pltpu.VMEM((64, D), bf16),
                pltpu.VMEM((48, D), bf16),
                pltpu.VMEM((48, D), bf16),
                dma((8,)),
                dma((SLOTS, 3)),
                dma((8, CHUNKS)),
                dma((8, CHUNKS)),
            ],
            compiler_params=pltpu.CompilerParams(
                collective_id=0, has_side_effects=True, vmem_limit_bytes=60 << 20
            ),
            cost_estimate=pl.CostEstimate(
                flops=6 * ROWS * D * H, bytes_accessed=6 * D * H + 4 * ROWS * D, transcendentals=ROWS * H
            ),
        )(x, w_gate, w_up, w_down)

    return jax.shard_map(
        step,
        mesh=mesh,
        in_specs=(P("dp", None), P(None, "tp"), P(None, "tp"), P("tp", None)),
        out_specs=P("dp", None),
        check_vma=False,
    )
```

```python
import jax
import jax.numpy as jnp
from jax import lax
from jax.experimental import pallas as pl
from jax.experimental.pallas import tpu as pltpu
from jax.sharding import PartitionSpec as P

MESH = pl.DeviceIdType.MESH
ROWS, D, H = 128, 12288, 4224
KB = 1536
COLS = ((0, 1536), (1536, 1536), (3072, 1152))
NB = 512
CHUNKS = D // NB
TWO = 0
LAGS_TWO = (1, 4, 7, 10, 13, 15)
LAGS_ONE = (1, 4, 7, 9)
SLOTS = 4
WIDTH = 1408
KS, TILES = D // KB, D // KB * (H // WIDTH)

def splits(width):
    return [(at, min(512, width - at)) for at in range(0, width, 512)]


def kernel(x_hbm, g_hbm, u_hbm, d_hbm, y, xv, hidden, acc_g, acc_u, ring, term, own, send_a, recv_a, send_b, recv_b,
           x_sem, ring_sem, send_sem, recv_sem):
    bf16, f32 = jnp.bfloat16, jnp.float32
    me = lax.axis_index("tp")
    place = lax.rem(me, 2), me // 4, lax.rem(me // 2, 2)

    def flip(p):
        return [1 - v if p >> b & 1 else v for v, b in zip(place, (2, 1, 0))]

    def device(p):
        core, x, y_ = flip(p)
        return 4 * x + 2 * y_ + core

    def piece(p):
        core, x, y_ = flip(p)
        return pl.ds(pl.multiple_of((4 * core + 2 * x + y_) * 16, 16), 16)

    barrier = pltpu.get_barrier_semaphore()
    for p in range(1, 8):
        pl.semaphore_signal(barrier, inc=1, device_id={"tp": device(p)}, device_id_type=MESH)

    def x_copy(p):
        return pltpu.make_async_copy(x_hbm.at[piece(p), :], xv.at[pl.ds(16 * p, 16), :], x_sem.at[p])

    def in_copy(w_hbm, t, slot):
        row = pl.multiple_of(lax.rem(t, KS) * KB, KB)
        col = pl.multiple_of(t // KS * WIDTH, 128)
        return pltpu.make_async_copy(
            w_hbm.at[pl.ds(row, KB), pl.ds(col, WIDTH)], ring.at[slot, :, pl.ds(0, WIDTH)], ring_sem.at[slot, 0]
        )

    def cols(c):
        return pl.ds(pl.multiple_of(c * NB, NB), NB)

    def down_copy(c, slot, r):
        at, depth = COLS[r]
        return pltpu.make_async_copy(
            d_hbm.at[pl.ds(at, depth), cols(c)], ring.at[slot, pl.ds(0, depth), pl.ds(r * NB, NB)], ring_sem.at[slot, r]
        )

    for p in range(8):
        x_copy(p).start()
    for t in range(SLOTS // 2):
        in_copy(g_hbm, t, 2 * t).start()
        in_copy(u_hbm, t, 2 * t + 1).start()
    for p in range(8):
        x_copy(p).wait()

    def project(t, _):
        kb = lax.rem(t, KS)

        @pl.when(kb == 0)
        def _():
            acc_g[...] = jnp.zeros_like(acc_g)
            acc_u[...] = jnp.zeros_like(acc_u)

        xk = xv[:, pl.ds(pl.multiple_of(kb * KB, KB), KB)]
        for which, (w_hbm, acc) in enumerate(((g_hbm, acc_g), (u_hbm, acc_u))):
            slot = 2 * lax.rem(t, SLOTS // 2) + which
            in_copy(w_hbm, t, slot).wait()
            for c, n in splits(WIDTH):
                acc[:, c : c + n] += jnp.dot(xk, ring[slot, :, c : c + n], preferred_element_type=f32)

            @pl.when(t < TILES - SLOTS // 2)
            def _(w_hbm=w_hbm, slot=slot):
                in_copy(w_hbm, t + SLOTS // 2, slot).start()

            @pl.when(t >= TILES - SLOTS // 2)
            def _(slot=slot):
                for r in range(3):
                    down_copy(slot, slot, r).start()

        @pl.when(kb == KS - 1)
        def _():
            for c, n in splits(WIDTH):
                at = pl.ds(pl.multiple_of(t // KS * WIDTH + c, 128), n)
                hidden[:, at] = (jax.nn.silu(acc_g[:, c : c + n]) * acc_u[:, c : c + n]).astype(bf16)

        return 0

    lax.fori_loop(0, TILES, project, 0)

    pl.semaphore_wait(barrier, 7)

    def copy(k, src, dst, c, p):
        return pltpu.make_async_remote_copy(
            src_ref=src, dst_ref=dst, send_sem=send_sem.at[k, c], recv_sem=recv_sem.at[k, c],
            device_id={"tp": device(p)}, device_id_type=MESH,
        )

    def axes_of(odd):
        return (1, 2) if odd else (2, 1)

    def pair_copy(c):
        return copy(0, send_a.at[:, cols(c)], recv_a.at[:, cols(c)], c, 4)

    def sum_copy(c, k, rows, p):
        return copy(k, send_b.at[rows, cols(c)], recv_b.at[rows, cols(c)], c, p)

    def first_copy(c, odd):
        return sum_copy(c, 1, pl.ds(0, 32), axes_of(odd)[0])

    def second_copy(c, odd):
        return sum_copy(c, 2, pl.ds(32, 16), axes_of(odd)[1])

    def three_copies(c, odd):
        a, b = axes_of(odd)
        return [sum_copy(c, k, pl.ds(16 * k - 16, 16), p) for k, p in ((3, 3), (1, b), (2, a))]

    def out_copy(c, k, owner, p):
        at = y.at[piece(owner), cols(c)]
        return copy(k, at, at, c, p)

    def two_copies(c, odd):
        a, b = axes_of(odd)
        return [out_copy(c, 4, 0, b), out_copy(c, 5, 0, a)]

    def back_copy(c, odd):
        a, b = axes_of(odd)
        return out_copy(c, 7, b, a)

    def all_copies(c):
        return [out_copy(c, 7, 0, 3), out_copy(c, 4, 0, 1), out_copy(c, 5, 0, 2)]

    def wide_copy(c):
        at = y.at[pl.ds(pl.multiple_of(place[0] * 64, 64), 64), cols(c)]
        return copy(6, at, at, c, 4)

    def compute(c, odd):
        slot = lax.rem(c, SLOTS)
        for r in range(3):
            down_copy(c, slot, r).wait()
        total = None
        for r, (at, depth) in enumerate(COLS):
            part = jnp.dot(
                hidden[:, at : at + depth], ring[slot, :depth, r * NB : (r + 1) * NB], preferred_element_type=f32
            )
            total = part if total is None else total + part
        term[...] = total

        @pl.when(c + SLOTS < CHUNKS)
        def _():
            for r in range(3):
                down_copy(c + SLOTS, slot, r).start()

        a, b = axes_of(odd)
        for q, p in enumerate((0, b, a, 3)):
            own[16 * q : 16 * q + 16, cols(c)] = term[16 * p : 16 * p + 16, :]
            send_a[16 * q : 16 * q + 16, cols(c)] = term[64 + 16 * p : 80 + 16 * p, :].astype(bf16)
        pair_copy(c).start()

    def start(copies):
        for one in copies:
            one.start()

    def pair_two(c, odd):
        pair_copy(c).wait_recv()
        total = own[:, cols(c)] + recv_a[:, cols(c)].astype(f32)
        send_b[:32, cols(c)] = total[32:].astype(bf16)
        own[:32, cols(c)] = total[:32]
        first_copy(c, odd).start()

    def first(c, odd):
        first_copy(c, odd).wait_recv()
        total = own[:32, cols(c)] + recv_b[:32, cols(c)].astype(f32)
        send_b[32:, cols(c)] = total[16:].astype(bf16)
        own[:16, cols(c)] = total[:16]
        second_copy(c, odd).start()

    def second(c, odd):
        second_copy(c, odd).wait_recv()
        y[piece(0), cols(c)] = (own[:16, cols(c)] + recv_b[32:, cols(c)].astype(f32)).astype(bf16)
        start(two_copies(c, odd))

    def back(c, odd):
        two_copies(c, odd)[0].wait_recv()
        back_copy(c, odd).start()

    def wide_two(c, odd):
        two_copies(c, odd)[1].wait_recv()
        back_copy(c, odd).wait_recv()
        wide_copy(c).start()

    def pair_one(c, odd):
        pair_copy(c).wait_recv()
        total = own[:, cols(c)] + recv_a[:, cols(c)].astype(f32)
        send_b[:, cols(c)] = total[16:].astype(bf16)
        own[:16, cols(c)] = total[:16]
        start(three_copies(c, odd))

    def three(c, odd):
        for one in three_copies(c, odd):
            one.wait_recv()
        total = own[:16, cols(c)]
        for q in range(3):
            total = total + recv_b[16 * q : 16 * q + 16, cols(c)].astype(f32)
        y[piece(0), cols(c)] = total.astype(bf16)
        start(all_copies(c))

    def wide_one(c, odd):
        for one in all_copies(c):
            one.wait_recv()
        wide_copy(c).start()

    def end(c, odd):
        wide_copy(c).wait_recv()

    stages = [(lag, f, 0, TWO) for lag, f in zip(LAGS_TWO, (pair_two, first, second, back, wide_two, end))]
    stages += [(lag, f, TWO, CHUNKS) for lag, f in zip(LAGS_ONE, (pair_one, three, wide_one, end))]
    stages = sorted((s for s in stages if s[2] < s[3]), key=lambda s: (s[0], -s[2]))

    def steps(lo, hi):
        def two_steps(t, _):
            for odd in (0, 1):
                i = 2 * t + odd
                if lo < CHUNKS:
                    compute(i, odd)
                for lag, stage, begin, stop in stages:
                    c, c_odd = i - lag, (odd + lag) % 2
                    if hi - 1 - lag < begin or lo - lag >= stop:
                        continue
                    if lo - lag >= begin and hi - 1 - lag < stop:
                        stage(c, c_odd)
                        continue

                    @pl.when((c >= begin) & (c < stop))
                    def _(stage=stage, c=c, c_odd=c_odd):
                        stage(c, c_odd)

            return 0

        lax.fori_loop(lo // 2, hi // 2, two_steps, 0)

    last = max(TWO - 1 + LAGS_TWO[-1] if TWO else 0, CHUNKS - 1 + LAGS_ONE[-1] if TWO < CHUNKS else 0) + 1
    steps(0, CHUNKS)
    steps(CHUNKS, last + last % 2)

    def drain(t, _):
        for odd in (0, 1):
            c = 2 * t + odd
            pair_copy(c).wait_send()
            wide_copy(c).wait_send()

            @pl.when(c < TWO)
            def _(c=c, odd=odd):
                for one in (first_copy(c, odd), second_copy(c, odd), *two_copies(c, odd), back_copy(c, odd)):
                    one.wait_send()

            @pl.when(c >= TWO)
            def _(c=c, odd=odd):
                for one in three_copies(c, odd) + all_copies(c):
                    one.wait_send()

        return 0

    lax.fori_loop(0, CHUNKS // 2, drain, 0)


def solution(mesh):
    bf16, f32 = jnp.bfloat16, jnp.float32

    def step(x, w_gate, w_up, w_down):
        dma = pltpu.SemaphoreType.DMA
        return pl.pallas_call(
            kernel,
            out_shape=pltpu.VMEM((ROWS, D), bf16),
            in_specs=[pl.BlockSpec(memory_space=pl.ANY)] * 4,
            out_specs=pl.BlockSpec(memory_space=pltpu.VMEM),
            scratch_shapes=[
                pltpu.VMEM((ROWS, D), bf16),
                pltpu.VMEM((ROWS, H), bf16),
                pltpu.VMEM((ROWS, WIDTH), f32),
                pltpu.VMEM((ROWS, WIDTH), f32),
                pltpu.VMEM((SLOTS, KB, KB), bf16),
                pltpu.VMEM((ROWS, NB), f32),
                pltpu.VMEM((64, D), f32),
                pltpu.VMEM((64, D), bf16),
                pltpu.VMEM((64, D), bf16),
                pltpu.VMEM((48, D), bf16),
                pltpu.VMEM((48, D), bf16),
                dma((8,)),
                dma((SLOTS, 3)),
                dma((8, CHUNKS)),
                dma((8, CHUNKS)),
            ],
            compiler_params=pltpu.CompilerParams(
                collective_id=0, has_side_effects=True, vmem_limit_bytes=60 << 20
            ),
            cost_estimate=pl.CostEstimate(
                flops=6 * ROWS * D * H, bytes_accessed=6 * D * H + 4 * ROWS * D, transcendentals=ROWS * H
            ),
        )(x, w_gate, w_up, w_down)

    return jax.shard_map(
        step,
        mesh=mesh,
        in_specs=(P("dp", None), P(None, "tp"), P(None, "tp"), P("tp", None)),
        out_specs=P("dp", None),
        check_vma=False,
    )
```

```python
import jax
import jax.numpy as jnp
from jax import lax
from jax.experimental import pallas as pl
from jax.experimental.pallas import tpu as pltpu
from jax.sharding import PartitionSpec as P

MESH = pl.DeviceIdType.MESH
ROWS, D, H = 128, 12288, 4224
KB = 1536
COLS = ((0, 1536), (1536, 1536), (3072, 1152))
NB = 512
CHUNKS = D // NB
TWO = 20
LAGS_TWO = (1, 4, 7, 10, 13, 15)
LAGS_ONE = (1, 5, 9, 11)
SLOTS = 4
WIDTH = 1408
KS, TILES = D // KB, D // KB * (H // WIDTH)

def splits(width):
    return [(at, min(512, width - at)) for at in range(0, width, 512)]


def kernel(x_hbm, g_hbm, u_hbm, d_hbm, y, xv, hidden, acc_g, acc_u, ring, term, own, send_a, recv_a, send_b, recv_b,
           x_sem, ring_sem, send_sem, recv_sem):
    bf16, f32 = jnp.bfloat16, jnp.float32
    me = lax.axis_index("tp")
    place = lax.rem(me, 2), me // 4, lax.rem(me // 2, 2)

    def flip(p):
        return [1 - v if p >> b & 1 else v for v, b in zip(place, (2, 1, 0))]

    def device(p):
        core, x, y_ = flip(p)
        return 4 * x + 2 * y_ + core

    def piece(p):
        core, x, y_ = flip(p)
        return pl.ds(pl.multiple_of((4 * core + 2 * x + y_) * 16, 16), 16)

    barrier = pltpu.get_barrier_semaphore()
    for p in range(1, 8):
        pl.semaphore_signal(barrier, inc=1, device_id={"tp": device(p)}, device_id_type=MESH)

    def x_copy(p):
        return pltpu.make_async_copy(x_hbm.at[piece(p), :], xv.at[pl.ds(16 * p, 16), :], x_sem.at[p])

    def in_copy(w_hbm, t, slot):
        row = pl.multiple_of(lax.rem(t, KS) * KB, KB)
        col = pl.multiple_of(t // KS * WIDTH, 128)
        return pltpu.make_async_copy(
            w_hbm.at[pl.ds(row, KB), pl.ds(col, WIDTH)], ring.at[slot, :, pl.ds(0, WIDTH)], ring_sem.at[slot, 0]
        )

    def cols(c):
        return pl.ds(pl.multiple_of(c * NB, NB), NB)

    def down_copy(c, slot, r):
        at, depth = COLS[r]
        return pltpu.make_async_copy(
            d_hbm.at[pl.ds(at, depth), cols(c)], ring.at[slot, pl.ds(0, depth), pl.ds(r * NB, NB)], ring_sem.at[slot, r]
        )

    for p in range(8):
        x_copy(p).start()
    for t in range(SLOTS // 2):
        in_copy(g_hbm, t, 2 * t).start()
        in_copy(u_hbm, t, 2 * t + 1).start()
    for p in range(8):
        x_copy(p).wait()

    def project(t, _):
        kb = lax.rem(t, KS)

        @pl.when(kb == 0)
        def _():
            acc_g[...] = jnp.zeros_like(acc_g)
            acc_u[...] = jnp.zeros_like(acc_u)

        xk = xv[:, pl.ds(pl.multiple_of(kb * KB, KB), KB)]
        for which, (w_hbm, acc) in enumerate(((g_hbm, acc_g), (u_hbm, acc_u))):
            slot = 2 * lax.rem(t, SLOTS // 2) + which
            in_copy(w_hbm, t, slot).wait()
            for c, n in splits(WIDTH):
                acc[:, c : c + n] += jnp.dot(xk, ring[slot, :, c : c + n], preferred_element_type=f32)

            @pl.when(t < TILES - SLOTS // 2)
            def _(w_hbm=w_hbm, slot=slot):
                in_copy(w_hbm, t + SLOTS // 2, slot).start()

            @pl.when(t >= TILES - SLOTS // 2)
            def _(slot=slot):
                for r in range(3):
                    down_copy(slot, slot, r).start()

        @pl.when(kb == KS - 1)
        def _():
            for c, n in splits(WIDTH):
                at = pl.ds(pl.multiple_of(t // KS * WIDTH + c, 128), n)
                hidden[:, at] = (jax.nn.silu(acc_g[:, c : c + n]) * acc_u[:, c : c + n]).astype(bf16)

        return 0

    lax.fori_loop(0, TILES, project, 0)

    pl.semaphore_wait(barrier, 7)

    def copy(k, src, dst, c, p):
        return pltpu.make_async_remote_copy(
            src_ref=src, dst_ref=dst, send_sem=send_sem.at[k, c], recv_sem=recv_sem.at[k, c],
            device_id={"tp": device(p)}, device_id_type=MESH,
        )

    def axes_of(odd):
        return (1, 2) if odd else (2, 1)

    def pair_copy(c):
        return copy(0, send_a.at[:, cols(c)], recv_a.at[:, cols(c)], c, 4)

    def sum_copy(c, k, rows, p):
        return copy(k, send_b.at[rows, cols(c)], recv_b.at[rows, cols(c)], c, p)

    def first_copy(c, odd):
        return sum_copy(c, 1, pl.ds(0, 32), axes_of(odd)[0])

    def second_copy(c, odd):
        return sum_copy(c, 2, pl.ds(32, 16), axes_of(odd)[1])

    def three_copies(c, odd):
        a, b = axes_of(odd)
        return [sum_copy(c, k, pl.ds(16 * k - 16, 16), p) for k, p in ((3, 3), (1, b), (2, a))]

    def out_copy(c, k, owner, p):
        at = y.at[piece(owner), cols(c)]
        return copy(k, at, at, c, p)

    def two_copies(c, odd):
        a, b = axes_of(odd)
        return [out_copy(c, 4, 0, b), out_copy(c, 5, 0, a)]

    def back_copy(c, odd):
        a, b = axes_of(odd)
        return out_copy(c, 7, b, a)

    def all_copies(c):
        return [out_copy(c, 7, 0, 3), out_copy(c, 4, 0, 1), out_copy(c, 5, 0, 2)]

    def wide_copy(c):
        at = y.at[pl.ds(pl.multiple_of(place[0] * 64, 64), 64), cols(c)]
        return copy(6, at, at, c, 4)

    def compute(c, odd):
        slot = lax.rem(c, SLOTS)
        total = None
        for r, (at, depth) in enumerate(COLS):
            down_copy(c, slot, r).wait()
            part = jnp.dot(
                hidden[:, at : at + depth], ring[slot, :depth, r * NB : (r + 1) * NB], preferred_element_type=f32
            )
            total = part if total is None else total + part
        term[...] = total

        @pl.when(c + SLOTS < CHUNKS)
        def _():
            for r in range(3):
                down_copy(c + SLOTS, slot, r).start()

        a, b = axes_of(odd)
        for q, p in enumerate((0, b, a, 3)):
            own[16 * q : 16 * q + 16, cols(c)] = term[16 * p : 16 * p + 16, :]
            send_a[16 * q : 16 * q + 16, cols(c)] = term[64 + 16 * p : 80 + 16 * p, :].astype(bf16)
        pair_copy(c).start()

    def start(copies):
        for one in copies:
            one.start()

    def pair_two(c, odd):
        pair_copy(c).wait_recv()
        total = own[:, cols(c)] + recv_a[:, cols(c)].astype(f32)
        send_b[:32, cols(c)] = total[32:].astype(bf16)
        own[:32, cols(c)] = total[:32]
        first_copy(c, odd).start()

    def first(c, odd):
        first_copy(c, odd).wait_recv()
        total = own[:32, cols(c)] + recv_b[:32, cols(c)].astype(f32)
        send_b[32:, cols(c)] = total[16:].astype(bf16)
        own[:16, cols(c)] = total[:16]
        second_copy(c, odd).start()

    def second(c, odd):
        second_copy(c, odd).wait_recv()
        y[piece(0), cols(c)] = (own[:16, cols(c)] + recv_b[32:, cols(c)].astype(f32)).astype(bf16)
        start(two_copies(c, odd))

    def back(c, odd):
        two_copies(c, odd)[0].wait_recv()
        back_copy(c, odd).start()

    def wide_two(c, odd):
        two_copies(c, odd)[1].wait_recv()
        back_copy(c, odd).wait_recv()
        wide_copy(c).start()

    def pair_one(c, odd):
        pair_copy(c).wait_recv()
        total = own[:, cols(c)] + recv_a[:, cols(c)].astype(f32)
        send_b[:, cols(c)] = total[16:].astype(bf16)
        own[:16, cols(c)] = total[:16]
        start(three_copies(c, odd))

    def three(c, odd):
        for one in three_copies(c, odd):
            one.wait_recv()
        total = own[:16, cols(c)]
        for q in range(3):
            total = total + recv_b[16 * q : 16 * q + 16, cols(c)].astype(f32)
        y[piece(0), cols(c)] = total.astype(bf16)
        start(all_copies(c))

    def wide_one(c, odd):
        for one in all_copies(c):
            one.wait_recv()
        wide_copy(c).start()

    def end(c, odd):
        wide_copy(c).wait_recv()

    stages = [(lag, f, 0, TWO) for lag, f in zip(LAGS_TWO, (pair_two, first, second, back, wide_two, end))]
    stages += [(lag, f, TWO, CHUNKS) for lag, f in zip(LAGS_ONE, (pair_one, three, wide_one, end))]
    stages.sort(key=lambda s: (s[0], -s[2]))

    def steps(lo, hi):
        def two_steps(t, _):
            for odd in (0, 1):
                i = 2 * t + odd
                if lo < CHUNKS:
                    compute(i, odd)
                for lag, stage, begin, stop in stages:
                    c, c_odd = i - lag, (odd + lag) % 2
                    if hi - 1 - lag < begin or lo - lag >= stop:
                        continue
                    if lo - lag >= begin and hi - 1 - lag < stop:
                        stage(c, c_odd)
                        continue

                    @pl.when((c >= begin) & (c < stop))
                    def _(stage=stage, c=c, c_odd=c_odd):
                        stage(c, c_odd)

            return 0

        lax.fori_loop(lo // 2, hi // 2, two_steps, 0)

    last = max(TWO - 1 + LAGS_TWO[-1] if TWO else 0, CHUNKS - 1 + LAGS_ONE[-1] if TWO < CHUNKS else 0) + 1
    steps(0, CHUNKS)
    steps(CHUNKS, last + last % 2)

    def drain(t, _):
        for odd in (0, 1):
            c = 2 * t + odd
            pair_copy(c).wait_send()
            wide_copy(c).wait_send()

            @pl.when(c < TWO)
            def _(c=c, odd=odd):
                for one in (first_copy(c, odd), second_copy(c, odd), *two_copies(c, odd), back_copy(c, odd)):
                    one.wait_send()

            @pl.when(c >= TWO)
            def _(c=c, odd=odd):
                for one in three_copies(c, odd) + all_copies(c):
                    one.wait_send()

        return 0

    lax.fori_loop(0, CHUNKS // 2, drain, 0)


def solution(mesh):
    bf16, f32 = jnp.bfloat16, jnp.float32

    def step(x, w_gate, w_up, w_down):
        dma = pltpu.SemaphoreType.DMA
        return pl.pallas_call(
            kernel,
            out_shape=pltpu.VMEM((ROWS, D), bf16),
            in_specs=[pl.BlockSpec(memory_space=pl.ANY)] * 4,
            out_specs=pl.BlockSpec(memory_space=pltpu.VMEM),
            scratch_shapes=[
                pltpu.VMEM((ROWS, D), bf16),
                pltpu.VMEM((ROWS, H), bf16),
                pltpu.VMEM((ROWS, WIDTH), f32),
                pltpu.VMEM((ROWS, WIDTH), f32),
                pltpu.VMEM((SLOTS, KB, KB), bf16),
                pltpu.VMEM((ROWS, NB), f32),
                pltpu.VMEM((64, D), f32),
                pltpu.VMEM((64, D), bf16),
                pltpu.VMEM((64, D), bf16),
                pltpu.VMEM((48, D), bf16),
                pltpu.VMEM((48, D), bf16),
                dma((8,)),
                dma((SLOTS, 3)),
                dma((8, CHUNKS)),
                dma((8, CHUNKS)),
            ],
            compiler_params=pltpu.CompilerParams(
                collective_id=0, has_side_effects=True, vmem_limit_bytes=60 << 20
            ),
            cost_estimate=pl.CostEstimate(
                flops=6 * ROWS * D * H, bytes_accessed=6 * D * H + 4 * ROWS * D, transcendentals=ROWS * H
            ),
        )(x, w_gate, w_up, w_down)

    return jax.shard_map(
        step,
        mesh=mesh,
        in_specs=(P("dp", None), P(None, "tp"), P(None, "tp"), P("tp", None)),
        out_specs=P("dp", None),
        check_vma=False,
    )
```
